256 devices in a mesh: pp: 4 (over x), cp: 64 (over z, y, core).
Axes of the slice: x: 4, y: 4, z: 8, core: 2. Of those that a mesh axis runs over, the one named last changes fastest.
Arguments:
- x_in: bfloat16 [4, 8192, 2048], P(None, 'cp'), may hold values from -60 to 80
- norm_gain: float32 [4, 2048], P('pp'), may hold values from 0.5 to 1.5
- w_qkv: bfloat16 [4, 2048, 3072], P('pp', 'cp'), may hold values from -0.13258252 to 1.307771
- w_out: bfloat16 [4, 2048, 2048], P('pp', 'cp'), may hold values from -0.125 to 0.125
- cycle_size: int32 [4], replicated, may hold values from 2 to 8, as said below
- token_pos: int32 [4, 8192], replicated, may hold values from 0 to 8191, as said below
- doc_starts: int32 [4, 128], replicated, may hold values from 0 to 8192, as said below
Outputs:
- layer_outputs: bfloat16 [4, 4, 8192, 2048], P('pp', None, 'cp')
The draws below stay inside these ranges and needn't reach their ends.
Inputs may be any that keep to these rules, and one draw needn't show every extreme that they name: `cycle_size`: powers of two dividing the devices of cp; some micro-batch has 8 and some has 2. `token_pos`: for a micro-batch with group size r, every aligned block of r * 128 slots holds each position of that block once. `doc_starts`: for a micro-batch with group size r and g below 64 / r, entry 2 g is g * r * 128 and entry 2 g + 1 either lies strictly inside that group's positions or is 8192, so each group holds one or two documents; the remaining entries are 8192.
All inputs are finite; a program needn't handle non-finite values.
Results may differ from the reference program's by a relative error of at most 0.0075.
Values may be sent and summed in bfloat16 or wider, within the bound.
A program may use at most 128 MiB of HBM per device.

```python
import math
import jax
import jax.numpy as jnp
from jax import lax

D = 2048
HEADS = 16
KV_HEADS = 4
HEAD_DIM = 128
T_DEV = 128
MICRO = 4
CYCLE_MAX = 8
LAYERS = 4
TOKENS = 8192
DOCS = 128
QKV_COLS = 3072


def cycle_draw(key):
    levels = CYCLE_MAX.bit_length() - 1
    exponent = jax.random.randint(key, (MICRO,), 1, levels + 1).astype(jnp.int32)
    sizes_drawn = jnp.left_shift(jnp.int32(1), exponent)
    chosen = jax.random.randint(jax.random.fold_in(key, 1), (), 0, MICRO)
    other = (chosen + jax.random.randint(jax.random.fold_in(key, 2), (), 1, MICRO)) % MICRO
    index = jnp.arange(MICRO)
    sizes_drawn = jnp.where(index == other, 2, sizes_drawn)
    return jnp.where(index == chosen, CYCLE_MAX, sizes_drawn).astype(jnp.int32)


def draw_cycle_size(key, part):
    return cycle_draw(jax.random.fold_in(key, 11))


def draw_token_pos(key, part):
    cycles = cycle_draw(jax.random.fold_in(key, 11))

    def one_row(row_key, cycle_devices):
        span = cycle_devices * T_DEV
        slots = jnp.arange(TOKENS, dtype=jnp.int32)
        groups = slots // span
        noise = jax.random.permutation(row_key, TOKENS).astype(jnp.int32)
        ordered = jnp.argsort(groups * TOKENS + noise, stable=True)
        return jnp.zeros((TOKENS,), jnp.int32).at[ordered].set(slots)
    row_keys = jax.random.split(jax.random.fold_in(key, 12), MICRO)
    return jax.vmap(one_row)(row_keys, cycles)


def draw_doc_starts(key, part):
    cycles = cycle_draw(jax.random.fold_in(key, 11))
    group_slots = DOCS // 2

    def one_row(row_key, cycle_devices):
        span = cycle_devices * T_DEV
        live_groups = group_slots // cycle_devices
        index = jnp.arange(group_slots, dtype=jnp.int32)
        inside = jax.random.randint(row_key, (group_slots,), 1, span).astype(jnp.int32)
        split_here = jax.random.randint(jax.random.fold_in(row_key, 5), (group_slots,), 0, 2) == 1
        first_pos = index * span
        second_pos = jnp.where(split_here, first_pos + inside, TOKENS)
        paired = jnp.stack([first_pos, second_pos], axis=1).reshape(-1)
        live = jnp.repeat(index < live_groups, 2)
        return jnp.where(live, paired, TOKENS).astype(jnp.int32)
    row_keys = jax.random.split(jax.random.fold_in(key, 13), MICRO)
    return jax.vmap(one_row)(row_keys, cycles)


def draw_x_in(key, part):
    base_draw = jnp.clip(jax.random.normal(jax.random.fold_in(key, 21), (MICRO, TOKENS, D), jnp.float32), -6.0, 6.0)
    return base_draw.astype(jnp.bfloat16)


def draw_w_qkv(key, part):
    base_draw = jnp.clip(jax.random.normal(jax.random.fold_in(key, 31), (LAYERS, D, QKV_COLS), jnp.float32), -6.0, 6.0) * D ** (-0.5)
    return base_draw.astype(jnp.bfloat16)


def block_levels(rng, extent, shards, smallest, top_value):
    def one(position, blocks):
        draws = jax.random.uniform(jax.random.fold_in(jax.random.fold_in(rng, 6), position), (blocks,), jnp.float32, smallest / len(shards), top_value / len(shards))
        return jnp.repeat(jnp.exp(draws), extent[position] // blocks).reshape((-1,) + (1,) * (len(extent) - position - 1))

    gain = one(*shards[0])
    for cut in shards[1:]:
        gain = gain * one(*cut)
    return gain


def centred(stream_key, extent, width, bound, cuts=(), held_as=jnp.bfloat16):
    gain = block_levels(stream_key, extent, cuts, -0.22, 0.18) if cuts else 1.0
    array = jax.random.normal(stream_key, extent, jnp.float32) * width * gain
    return jnp.minimum(jnp.maximum(array, -bound), bound).astype(held_as)


def setup_inputs(seed: int = 0) -> dict:
    seeds = jax.random.split(jax.random.key(seed), 8)
    return {
        "x_in": draw_x_in(jax.random.fold_in(seeds[7], 71), 0),
        "norm_gain": jnp.clip(1.0 + 0.1 * jax.random.normal(seeds[1], (LAYERS, D), jnp.float32), 0.5, 1.5),
        "w_qkv": draw_w_qkv(jax.random.fold_in(seeds[7], 71), 0),
        "w_out": centred(seeds[3], (LAYERS, HEADS * HEAD_DIM, D), (HEADS * HEAD_DIM) ** -0.5, 0.125, ((0, 4), (1, 64))),
        "cycle_size": draw_cycle_size(jax.random.fold_in(seeds[7], 71), 0),
        "token_pos": draw_token_pos(jax.random.fold_in(seeds[7], 71), 0),
        "doc_starts": draw_doc_starts(jax.random.fold_in(seeds[7], 71), 0),
    }


epsilon = 1e-05
rope_base = 500000.0

def rotate(values, relative):
    half_dim = values.shape[-1] // 2
    frequency_index = jnp.arange(half_dim, dtype=jnp.float32)
    inverse = jnp.power(jnp.float32(rope_base), -2.0 * frequency_index / values.shape[-1])
    angles = relative.astype(jnp.float32)[:, None] * inverse[None, :]
    cosine = jnp.cos(angles)[:, None, :]
    sine_part = jnp.sin(angles)[:, None, :]
    first_half = values[..., :half_dim]
    second_half = values[..., half_dim:]
    return jnp.concatenate([first_half * cosine - second_half * sine_part, second_half * cosine + first_half * sine_part], axis=-1)

def doc_begin(positions, starts):
    at_or_below = starts[None, :] <= positions[:, None]
    return lax.optimization_barrier(jnp.max(jnp.where(at_or_below, starts[None, :], 0), axis=1)).astype(jnp.int32)

def layer_forward(hidden, gain_row, qkv_weight, out_weight, positions, starts, cycle_devices):
    widened = hidden.astype(jnp.float32)
    mean_square = lax.optimization_barrier(jnp.mean(widened * widened, axis=-1, keepdims=True))
    normed = (widened * lax.rsqrt(mean_square + epsilon) * gain_row.astype(jnp.float32)).astype(jnp.bfloat16)
    projected = jnp.dot(normed, qkv_weight, preferred_element_type=jnp.float32)
    query_cols = HEADS * HEAD_DIM
    key_cols = KV_HEADS * HEAD_DIM
    begins = doc_begin(positions, starts)
    relative = positions - begins
    queries = rotate(projected[:, :query_cols].reshape(-1, HEADS, HEAD_DIM), relative).astype(jnp.bfloat16)
    keys_all = rotate(projected[:, query_cols:query_cols + key_cols].reshape(-1, KV_HEADS, HEAD_DIM), relative).astype(jnp.bfloat16)
    values_all = projected[:, query_cols + key_cols:].reshape(-1, KV_HEADS, HEAD_DIM).astype(jnp.bfloat16)
    groups = positions // (cycle_devices * T_DEV)
    window = CYCLE_MAX * T_DEV
    block_rows = math.gcd(window, 512)
    block_count = TOKENS // block_rows

    def attend(pieces):
        block_queries, block_pos, block_begin, block_group, block_number = pieces
        window_start = (block_number * block_rows // window * window).astype(jnp.int32)
        near_keys = lax.dynamic_slice_in_dim(keys_all, window_start, window, 0)
        near_values = lax.dynamic_slice_in_dim(values_all, window_start, window, 0)
        near_pos = lax.dynamic_slice_in_dim(positions, window_start, window, 0)
        near_begin = lax.dynamic_slice_in_dim(begins, window_start, window, 0)
        near_group = lax.dynamic_slice_in_dim(groups, window_start, window, 0)
        grouped = block_queries.astype(jnp.float32).reshape(block_rows, KV_HEADS, HEADS // KV_HEADS, HEAD_DIM)
        scores = jnp.einsum('bkgd,skd->kgbs', grouped, near_keys.astype(jnp.float32)) * HEAD_DIM ** (-0.5)
        visible = (block_group[:, None] == near_group[None, :]) & (block_begin[:, None] == near_begin[None, :]) & (near_pos[None, :] <= block_pos[:, None])
        scores = jnp.where(visible[None, None], scores, -1e+30)
        row_max = lax.optimization_barrier(jnp.max(scores, axis=-1, keepdims=True))
        weights_exp = jnp.exp(scores - row_max)
        row_sum = lax.optimization_barrier(jnp.sum(weights_exp, axis=-1, keepdims=True))
        rounded = lax.optimization_barrier(weights_exp.astype(jnp.bfloat16)).astype(jnp.float32)
        combined = jnp.einsum('kgbs,skd->kgbd', rounded, near_values.astype(jnp.float32)) / row_sum
        return jnp.transpose(combined, (2, 0, 1, 3)).reshape(block_rows, query_cols).astype(jnp.bfloat16)
    attended = lax.map(attend, (queries.reshape(block_count, block_rows, HEADS, HEAD_DIM), positions.reshape(block_count, block_rows), begins.reshape(block_count, block_rows), groups.reshape(block_count, block_rows), jnp.arange(block_count, dtype=jnp.int32)))
    attended = attended.reshape(TOKENS, query_cols)
    output = jnp.dot(attended, out_weight, preferred_element_type=jnp.float32)
    return (widened + output).astype(jnp.bfloat16)

def reference(x_in, norm_gain, w_qkv, w_out, cycle_size, token_pos, doc_starts):
    per_micro = []
    for micro_index in range(MICRO):
        hidden = x_in[micro_index]
        layer_rows = []
        for layer_index in range(LAYERS):
            hidden = layer_forward(hidden, norm_gain[layer_index], w_qkv[layer_index], w_out[layer_index], token_pos[micro_index], doc_starts[micro_index], cycle_size[micro_index])
            layer_rows.append(hidden)
        per_micro.append(jnp.stack(layer_rows))
    return jnp.stack(per_micro, axis=1)
```

```python
import functools
import math

import jax
import jax.numpy as jnp
from jax import lax
from jax.experimental import pallas as pl
from jax.experimental.pallas import tpu as pltpu
from jax.sharding import PartitionSpec as P

MESH = pl.DeviceIdType.MESH
HEAD_DIM = 128
MICRO = 4
SECTIONS = 4
NY = 4
NZ = 8
BLK = 64
ROWS = 256
HALF = 1024
KVC = 512
EPS = 1e-05
ROPE_BASE = 500000.0
QSCALE = HEAD_DIM ** (-0.5) * math.log2(math.e)
N_GATHER = 176


class Comm:
    def __init__(self, ssem, rsem, home):
        self.ssem, self.rsem, self.home = ssem, rsem, home
        self.count = 0
        self.sent = []

    def make(self, src, dst, idx, dev):
        return pltpu.make_async_remote_copy(
            src_ref=src, dst_ref=dst, send_sem=self.ssem.at[idx], recv_sem=self.rsem.at[idx],
            device_id=dev, device_id_type=MESH)

    def send(self, ref, dev, dst=None):
        idx = self.count
        self.count += 1
        copy = self.make(ref, ref if dst is None else dst, idx, dev)
        copy.start()
        self.sent.append(copy)
        return idx

    def wait(self, ref, idx):
        self.make(ref, ref, idx, self.home).wait_recv()

    def drain(self):
        for copy in self.sent:
            copy.wait_send()
        self.sent = []


def kernel(wh_ref, x_ref, cos_ref, sin_ref, qpos_ref, qbeg_ref, kpos_ref, out_ref,
           wkv, wq, woa, wob, hid, kvb, qb, att, outb, bias,
           g_ssem, g_rsem, lsem, x_ssem, x_rsem, d_ssem, d_rsem, k_ssem, k_rsem, a_ssem, a_rsem, o_ssem, o_rsem):
    s = lax.axis_index("pp")
    cp = lax.axis_index("cp")
    c = cp % 2
    y = (cp // 2) % NY
    z = cp // (2 * NY)
    ym, yp, y2 = (y + NY - 1) % NY, (y + 1) % NY, (y + 2) % NY

    def dev(yy, zz, cc):
        return (s, (zz * NY + yy) * 2 + cc)

    sib = dev(y, z, 1 - c)
    dyp, dym = dev(yp, z, c), dev(ym, z, c)
    dzp, dzm = dev(y, (z + 1) % NZ, c), dev(y, (z + NZ - 1) % NZ, c)
    xnext, xprev = ((s + 1) % SECTIONS, cp), ((s + SECTIONS - 1) % SECTIONS, cp)

    barrier = pltpu.get_barrier_semaphore()
    for d in (sib, dyp, dym, dzp, dzm, xnext, xprev):
        pl.semaphore_signal(barrier, inc=1, device_id=d, device_id_type=MESH)
    pl.semaphore_wait(barrier, 7)

    comm = Comm(g_ssem, g_rsem, sib)
    mine = pl.ds(pl.multiple_of(c * 32, 32), 32)
    other = pl.ds(pl.multiple_of((1 - c) * 32, 32), 32)
    cols = ((wkv, 0, 512), (wq, 512, 1024), (woa, 1536, 512), (wob, 2048, 512))
    local, sibs = [], []
    for i, (w, at, n) in enumerate(cols):
        sibs.append(comm.send(wh_ref.at[1 - c, :, at:at + n], sib, dst=w.at[z, y, mine]))
        cpy = pltpu.make_async_copy(wh_ref.at[c, :, at:at + n], w.at[z, y, mine], lsem.at[i])
        cpy.start()
        local.append(cpy)

    toks = pl.ds(pl.multiple_of(c * 128, 128), 128)
    toks_o = pl.ds(pl.multiple_of((1 - c) * 128, 128), 128)

    def own_ready(i):
        w = cols[i][0]
        local[i].wait()
        comm.wait(w.at[z, y, other], sibs[i])

    def flood(wa, wb):
        lo, hi = pl.ds(0, 32), pl.ds(32, 32)
        a_p = comm.send(wa.at[z, y], dyp)
        a_m = comm.send(wa.at[z, y], dym)
        bz_p = comm.send(wb.at[z, y], dzp)
        bz_m = comm.send(wb.at[z, y], dzm)
        by = {}
        by[0] = (comm.send(wb.at[z, y], dyp), comm.send(wb.at[z, y], dym))
        az = {}
        az[0] = (comm.send(wa.at[z, y], dzp), comm.send(wa.at[z, y], dzm))
        comm.wait(wa.at[z, ym], a_p)
        f_p = comm.send(wa.at[z, ym, lo], dyp)
        az[1] = (comm.send(wa.at[z, ym], dzp), comm.send(wa.at[z, ym], dzm))
        comm.wait(wa.at[z, yp], a_m)
        f_m = comm.send(wa.at[z, yp, hi], dym)
        az[2] = (comm.send(wa.at[z, yp], dzp), comm.send(wa.at[z, yp], dzm))
        ycols = (y, ym, yp, y2)
        halves = []

        def y_arrivals(zz, key):
            i_p, i_m = by[key]
            comm.wait(wb.at[zz, ym], i_p)
            h_p = comm.send(wb.at[zz, ym, lo], dyp)
            comm.wait(wb.at[zz, yp], i_m)
            h_m = comm.send(wb.at[zz, yp, hi], dym)
            halves.append((zz, h_p, h_m))

        for d in (1, 2, 3):
            zm, zp = (z + NZ - d) % NZ, (z + d) % NZ
            part_p, part_m = (lo, hi) if d == 3 else (slice(None), slice(None))
            comm.wait(wb.at[zm, y], bz_p)
            n_p = comm.send(wb.at[zm, y, part_p], dzp)
            by[-d] = (comm.send(wb.at[zm, y], dyp), comm.send(wb.at[zm, y], dym))
            comm.wait(wb.at[zp, y], bz_m)
            n_m = comm.send(wb.at[zp, y, part_m], dzm)
            by[d] = (comm.send(wb.at[zp, y], dyp), comm.send(wb.at[zp, y], dym))
            bz_p, bz_m = n_p, n_m
            if d == 1:
                comm.wait(wa.at[z, y2, lo], f_p)
                comm.wait(wa.at[z, y2, hi], f_m)
                az[3] = (comm.send(wa.at[z, y2], dzp), comm.send(wa.at[z, y2], dzm))
            nxt = {}
            for k, yy in enumerate(ycols):
                comm.wait(wa.at[zm, yy], az[k][0])
                q_p = comm.send(wa.at[zm, yy, part_p], dzp)
                comm.wait(wa.at[zp, yy], az[k][1])
                q_m = comm.send(wa.at[zp, yy, part_m], dzm)
                nxt[k] = (q_p, q_m)
            az = nxt
            if d == 1:
                y_arrivals(z, 0)
            else:
                y_arrivals((z + NZ - d + 1) % NZ, -(d - 1))
                y_arrivals((z + d - 1) % NZ, d - 1)
        z4 = (z + 4) % NZ
        comm.wait(wb.at[z4, y, lo], bz_p)
        comm.wait(wb.at[z4, y, hi], bz_m)
        by[4] = (comm.send(wb.at[z4, y], dyp), comm.send(wb.at[z4, y], dym))
        for k, yy in enumerate(ycols):
            comm.wait(wa.at[z4, yy, lo], az[k][0])
            comm.wait(wa.at[z4, yy, hi], az[k][1])
        y_arrivals((z + NZ - 3) % NZ, -3)
        y_arrivals((z + 3) % NZ, 3)
        y_arrivals(z4, 4)
        for zz, h_p, h_m in halves:
            comm.wait(wb.at[zz, y2, lo], h_p)
            comm.wait(wb.at[zz, y2, hi], h_m)

    def rcopy(src, dst, ss, rs, d):
        return pltpu.make_async_remote_copy(src_ref=src, dst_ref=dst, send_sem=ss, recv_sem=rs,
                                            device_id=d, device_id_type=MESH)

    def x_local(m, h):
        return pltpu.make_async_copy(x_ref.at[m, :, h * HALF:(h + 1) * HALF], hid.at[m, h, toks], x_rsem.at[m, h])

    def x_sib(m, h):
        return rcopy(hid.at[m, h, toks], hid.at[m, h, toks], d_ssem.at[m, h], d_rsem.at[m, h], sib)

    def x_sib_in(m, h):
        return rcopy(hid.at[m, h, toks_o], hid.at[m, h, toks_o], d_ssem.at[m, h], d_rsem.at[m, h], sib)

    @pl.when(s == 0)
    def _():
        for m in range(MICRO):
            for h in range(2):
                x_local(m, h).start()

    own_ready(0)
    own_ready(1)

    @pl.when(s == 0)
    def _():
        for m in range(MICRO):
            for h in range(2):
                x_local(m, h).wait()
                x_sib(m, h).start()

    flood(wkv, wq)
    own_ready(2)
    own_ready(3)
    flood(woa, wob)

    @pl.when(s == 0)
    def _():
        for m in range(MICRO):
            for h in range(2):
                x_sib(m, h).wait_send()
                x_sib_in(m, h).wait_recv()

    def h_in(m):
        return rcopy(hid.at[m, c], hid.at[m, c], x_ssem.at[m], x_rsem.at[m, 0], xprev)

    def h_fwd(m):
        return rcopy(hid.at[m, c], hid.at[m, c], d_ssem.at[m, 0], d_rsem.at[m, 0], sib)

    def h_fwd_in(m):
        return rcopy(hid.at[m, 1 - c], hid.at[m, 1 - c], d_ssem.at[m, 0], d_rsem.at[m, 0], sib)

    def kv_out(m, i):
        return rcopy(kvb.at[m, y], kvb.at[m, y], k_ssem.at[m, i], k_rsem.at[m, i], (dyp, dym)[i])

    def kv_in(m, i):
        ref = kvb.at[m, (ym, yp)[i]]
        return rcopy(ref, ref, k_ssem.at[m, i], k_rsem.at[m, i], sib)

    def kv_half(m, i):
        ref = kvb.at[m, (ym, yp)[i], pl.ds(128 * i, 128)]
        return rcopy(ref, ref, k_ssem.at[m, 2 + i], k_rsem.at[m, 2 + i], (dyp, dym)[i])

    def kv_half_in(m, i):
        ref = kvb.at[m, y2, pl.ds(128 * i, 128)]
        return rcopy(ref, ref, k_ssem.at[m, 2 + i], k_rsem.at[m, 2 + i], sib)

    def rope(v, cos, sin):
        return v * cos + pltpu.roll(v, 64, 1) * sin

    def stage1(m):
        @pl.when(s > 0)
        def _():
            h_in(m).wait_recv()
            h_fwd(m).start()
            h_fwd_in(m).wait_recv()
            h_fwd(m).wait_send()

        h0 = hid[m, 0]
        h1 = hid[m, 1]
        f0, f1 = h0.astype(jnp.float32), h1.astype(jnp.float32)
        ms = jnp.sum(f0 * f0 + f1 * f1, axis=1, keepdims=True) * (1.0 / 2048.0)
        r = lax.rsqrt(ms + EPS)
        cos = cos_ref[m]
        sin = sin_ref[m]
        kv = jnp.dot(h0, wkv[0:4].reshape(HALF, KVC), preferred_element_type=jnp.float32)
        kv += jnp.dot(h1, wkv[4:8].reshape(HALF, KVC), preferred_element_type=jnp.float32)
        kv = kv * r
        for j in range(2):
            kvb[m, y, :, j * 128:(j + 1) * 128] = rope(kv[:, j * 128:(j + 1) * 128], cos, sin).astype(jnp.bfloat16)
        kvb[m, y, :, 256:512] = kv[:, 256:512].astype(jnp.bfloat16)
        kv_out(m, 0).start()
        kv_out(m, 1).start()
        rq = r * QSCALE
        for n in range(2):
            q = jnp.dot(h0, wq[0:4, :, :, n * 512:(n + 1) * 512].reshape(HALF, 512), preferred_element_type=jnp.float32)
            q += jnp.dot(h1, wq[4:8, :, :, n * 512:(n + 1) * 512].reshape(HALF, 512), preferred_element_type=jnp.float32)
            q = q * rq
            for j in range(4):
                h = n * 4 + j
                qb[m % 2, :, h * 128:(h + 1) * 128] = rope(q[:, j * 128:(j + 1) * 128], cos, sin).astype(jnp.bfloat16)
        for i in range(2):
            kv_in(m, i).wait_recv()
            kv_half(m, i).start()

    def attn_head(m, h):
        j = h // 4
        k = kvb[m, :, :, pl.ds(pl.multiple_of(j * 128, 128), 128)].reshape(4 * ROWS, HEAD_DIM)
        v = kvb[m, :, :, pl.ds(pl.multiple_of(256 + j * 128, 128), 128)].reshape(4 * ROWS, HEAD_DIM)
        at = pl.ds(pl.multiple_of(h * 128, 128), 128)
        q = qb[m % 2, :, at]
        sc = lax.dot_general(q, k, (((1,), (1,)), ((), ())), preferred_element_type=jnp.float32)
        sc = sc + bias[...]
        mx = jnp.max(sc, axis=1, keepdims=True)
        p = jnp.exp2(sc - mx)
        total = jnp.sum(p, axis=1, keepdims=True)
        o = jnp.dot(p.astype(jnp.bfloat16), v, preferred_element_type=jnp.float32)
        att[m, c, :, at] = (o / total).astype(jnp.bfloat16)

    def a_send(m, j):
        ref = att.at[m, c, :, j * 512:(j + 1) * 512]
        return rcopy(ref, ref, a_ssem.at[m, j], a_rsem.at[m, j], sib)

    def a_in(m, j):
        ref = att.at[m, 1 - c, :, j * 512:(j + 1) * 512]
        return rcopy(ref, ref, a_ssem.at[m, j], a_rsem.at[m, j], sib)

    def x_send(m):
        return rcopy(outb.at[m], hid.at[m, c], x_ssem.at[m], x_rsem.at[m, 0], xnext)

    out_cols = pl.ds(pl.multiple_of(c * HALF, HALF), HALF)
    out_cols_o = pl.ds(pl.multiple_of((1 - c) * HALF, HALF), HALF)

    def o_local(m):
        return pltpu.make_async_copy(outb.at[m, toks], out_ref.at[0, m, :, out_cols], lsem.at[4 + m])

    def o_sib(m):
        return rcopy(outb.at[m, toks_o], out_ref.at[0, m, :, out_cols], o_ssem.at[m], o_rsem.at[m], sib)

    def o_sib_in(m):
        ref = out_ref.at[0, m, :, out_cols_o]
        return rcopy(ref, ref, o_ssem.at[m], o_rsem.at[m], sib)

    def stage2(m):
        kp = kpos_ref[m]
        bias[...] = jnp.where((kp >= qbeg_ref[m]) & (kp <= qpos_ref[m]), 0.0, -1e30)
        for i in range(2):
            kv_half_in(m, i).wait_recv()
        for j in range(2):
            def head_pair(i, _):
                attn_head(m, j * 4 + i * 2)
                attn_head(m, j * 4 + i * 2 + 1)
                return 0
            lax.fori_loop(0, 2, head_pair, 0)
            a_send(m, j).start()
        for j in range(2):
            a_in(m, j).wait_recv()
        for n, w in enumerate((woa, wob)):
            o = jnp.dot(att[m, 0], w[0:4].reshape(HALF, 512), preferred_element_type=jnp.float32)
            o += jnp.dot(att[m, 1], w[4:8].reshape(HALF, 512), preferred_element_type=jnp.float32)
            o += hid[m, c, :, n * 512:(n + 1) * 512].astype(jnp.float32)
            outb[m, :, n * 512:(n + 1) * 512] = o.astype(jnp.bfloat16)

        @pl.when(s < SECTIONS - 1)
        def _():
            x_send(m).start()
        o_sib(m).start()
        o_local(m).start()

    def step(i, _):
        @pl.when(i < MICRO)
        def _():
            stage1(i)

        @pl.when(i > 0)
        def _():
            stage2(i - 1)
        return 0

    lax.fori_loop(0, MICRO + 1, step, 0)

    comm.drain()
    for m in range(MICRO):
        @pl.when(s < SECTIONS - 1)
        def _():
            x_send(m).wait_send()
        for i in range(2):
            kv_out(m, i).wait_send()
            kv_half(m, i).wait_send()
            a_send(m, i).wait_send()
        o_local(m).wait()
        o_sib(m).wait_send()
        o_sib_in(m).wait_recv()


def body(x_in, norm_gain, w_qkv, w_out, cycle_size, token_pos, doc_starts):
    cp = lax.axis_index("cp")
    chip = cp // 2
    gain = lax.dynamic_slice_in_dim(norm_gain[0], cp * 32, 32)
    wg = (w_qkv[0].astype(jnp.float32) * gain[:, None]).astype(jnp.bfloat16)
    wo = w_out[0]
    parts = []
    for c in range(2):
        parts.append(jnp.concatenate([
            wg[:, 2048 + 256 * c:2048 + 256 * (c + 1)], wg[:, 2560 + 256 * c:2560 + 256 * (c + 1)],
            wg[:, HALF * c:HALF * (c + 1)], wo[:, HALF * c:HALF * (c + 1)]], axis=1))
    wh = jnp.stack(parts)
    qpos = lax.dynamic_slice_in_dim(token_pos, chip * ROWS, ROWS, 1)
    kpos = lax.dynamic_slice_in_dim(token_pos, (cp // 8) * 4 * ROWS, 4 * ROWS, 1)
    starts = doc_starts[:, None, :]
    qbeg = jnp.max(jnp.where(starts <= qpos[:, :, None], starts, 0), axis=-1)
    inverse = jnp.power(jnp.float32(ROPE_BASE), -2.0 * jnp.arange(64, dtype=jnp.float32) / HEAD_DIM)
    angles = (qpos - qbeg).astype(jnp.float32)[:, :, None] * inverse[None, None, :]
    cos, sin = jnp.cos(angles), jnp.sin(angles)
    cos = jnp.concatenate([cos, cos], axis=-1)
    sin = jnp.concatenate([-sin, sin], axis=-1)
    vm = pl.BlockSpec(memory_space=pltpu.VMEM)
    anyspace = pl.BlockSpec(memory_space=pl.ANY)
    bf = jnp.bfloat16
    dma = pltpu.SemaphoreType.DMA
    return pl.pallas_call(
        kernel,
        name="relay",
        out_shape=jax.ShapeDtypeStruct((1, MICRO, 128, 2 * HALF), bf),
        in_specs=[vm, anyspace, vm, vm, vm, vm, vm],
        out_specs=anyspace,
        scratch_shapes=[
            pltpu.VMEM((NZ, NY, BLK, KVC), bf), pltpu.VMEM((NZ, NY, BLK, HALF), bf),
            pltpu.VMEM((NZ, NY, BLK, KVC), bf), pltpu.VMEM((NZ, NY, BLK, KVC), bf),
            pltpu.VMEM((MICRO, 2, ROWS, HALF), bf),
            pltpu.VMEM((MICRO, NY, ROWS, KVC), bf),
            pltpu.VMEM((2, ROWS, HALF), bf),
            pltpu.VMEM((MICRO, 2, ROWS, HALF), bf),
            pltpu.VMEM((MICRO, ROWS, HALF), bf),
            pltpu.VMEM((ROWS, 4 * ROWS), jnp.float32),
            dma((N_GATHER,)), dma((N_GATHER,)), dma((8,)),
            dma((MICRO,)), dma((MICRO, 2)), dma((MICRO, 2)), dma((MICRO, 2)),
            dma((MICRO, 4)), dma((MICRO, 4)), dma((MICRO, 2)), dma((MICRO, 2)), dma((MICRO,)), dma((MICRO,)),
        ],
        compiler_params=pltpu.CompilerParams(
            collective_id=0, has_side_effects=True, vmem_limit_bytes=60 * 1024 * 1024),
    )(wh, x_in, cos, sin, qpos[:, :, None], qbeg[:, :, None], kpos[:, None, :])


def solution(mesh):
    in_specs = (P(None, "cp", None), P("pp", None), P("pp", "cp", None), P("pp", "cp", None), P(), P(), P())
    return jax.shard_map(body, mesh=mesh, in_specs=in_specs, out_specs=P("pp", None, "cp", None), check_vma=False)
```

```python
import functools
import math

import jax
import jax.numpy as jnp
from jax import lax
from jax.experimental import pallas as pl
from jax.experimental.pallas import tpu as pltpu
from jax.sharding import PartitionSpec as P

MESH = pl.DeviceIdType.MESH
HEAD_DIM = 128
MICRO = 4
SECTIONS = 4
NY = 4
NZ = 8
BLK = 64
ROWS = 256
HALF = 1024
KVC = 512
EPS = 1e-05
ROPE_BASE = 500000.0
QSCALE = HEAD_DIM ** (-0.5) * math.log2(math.e)
N_GATHER = 200
OAC = 640
OBC = 384
STEP = 128


class Comm:
    def __init__(self, ssem, rsem, home):
        self.ssem, self.rsem, self.home = ssem, rsem, home
        self.count = 0
        self.sent = []

    def make(self, src, dst, idx, dev):
        return pltpu.make_async_remote_copy(
            src_ref=src, dst_ref=dst, send_sem=self.ssem.at[idx], recv_sem=self.rsem.at[idx],
            device_id=dev, device_id_type=MESH)

    def send(self, ref, dev, dst=None):
        idx = self.count
        self.count += 1
        copy = self.make(ref, ref if dst is None else dst, idx, dev)
        copy.start()
        self.sent.append(copy)
        return idx

    def wait(self, ref, idx):
        self.make(ref, ref, idx, self.home).wait_recv()

    def drain(self):
        for copy in self.sent:
            copy.wait_send()
        self.sent = []


def kernel(wqkv_ref, wout_ref, gain_ref, pos_ref, doc_ref, inv_ref, x_ref, out_ref,
           wkv, wq0, wq1, woa, wob, stage, hid, kvb, qb, att, outb, cos_t, sin_t, qpos_t, qbeg_t, kpos_t,
           g_ssem, g_rsem, x_ssem, x_rsem, d_ssem, d_rsem, k_ssem, k_rsem, a_ssem, a_rsem, o_ssem, o_rsem, l_sem):
    s = lax.axis_index("pp")
    cp = lax.axis_index("cp")
    c = cp % 2
    chip = cp // 2
    y = chip % NY
    z = chip // NY
    ym, yp, y2 = (y + NY - 1) % NY, (y + 1) % NY, (y + 2) % NY

    def dev(yy, zz, cc):
        return (s, (zz * NY + yy) * 2 + cc)

    sib = dev(y, z, 1 - c)
    dyp, dym = dev(yp, z, c), dev(ym, z, c)
    dzp, dzm = dev(y, (z + 1) % NZ, c), dev(y, (z + NZ - 1) % NZ, c)
    xnext, xprev = ((s + 1) % SECTIONS, cp), ((s + SECTIONS - 1) % SECTIONS, cp)
    neighbours = (sib, dyp, dym, dzp, dzm, xnext, xprev)

    barrier = pltpu.get_barrier_semaphore()
    for d in neighbours:
        pl.semaphore_signal(barrier, inc=1, device_id=d, device_id_type=MESH)

    mine = pl.ds(pl.multiple_of(c * 32, 32), 32)
    other = pl.ds(pl.multiple_of((1 - c) * 32, 32), 32)
    toks = pl.ds(pl.multiple_of(c * STEP, STEP), STEP)
    toks_o = pl.ds(pl.multiple_of((1 - c) * STEP, STEP), STEP)

    def rcopy(src, dst, ss, rs, d):
        return pltpu.make_async_remote_copy(src_ref=src, dst_ref=dst, send_sem=ss, recv_sem=rs,
                                            device_id=d, device_id_type=MESH)

    def x_local(m, h):
        return pltpu.make_async_copy(x_ref.at[m, :, h * HALF:(h + 1) * HALF], hid.at[m, h, toks], x_rsem.at[m, h])

    def x_sib(m, h):
        return rcopy(hid.at[m, h, toks], hid.at[m, h, toks], d_ssem.at[m, h], d_rsem.at[m, h], sib)

    def x_sib_in(m, h):
        return rcopy(hid.at[m, h, toks_o], hid.at[m, h, toks_o], d_ssem.at[m, h], d_rsem.at[m, h], sib)

    @pl.when(s == 0)
    def _():
        for m in range(MICRO):
            for h in range(2):
                x_local(m, h).start()

    at128 = pl.ds(pl.multiple_of(cp // 4 * 128, 128), 128)
    g_row = jnp.broadcast_to(gain_ref[0:1, at128], (32, 128))
    lane = lax.broadcasted_iota(jnp.int32, (32, 128), 1)
    sub = lax.broadcasted_iota(jnp.int32, (32, 128), 0)
    g_col = jnp.sum(jnp.where(lane == sub + cp % 4 * 32, g_row, 0.0), axis=1, keepdims=True)
    for cc in range(2):
        for src_at, dst_at, n in ((2048 + 256 * cc, 0, 256), (2560 + 256 * cc, 256, 256), (HALF * cc, 512, HALF)):
            part = wqkv_ref[0, :, src_at:src_at + n].astype(jnp.float32) * g_col
            stage[cc, :, dst_at:dst_at + n] = part.astype(jnp.bfloat16)
        stage[cc, :, 1536:2560] = wout_ref[0, :, HALF * cc:HALF * (cc + 1)]
    cols = ((wkv, 0, 512), (wq0, 512, 512), (wq1, 1024, 512), (woa, 1536, OAC), (wob, 1536 + OAC, OBC))
    for w, at, n in cols:
        w[z, y, mine, :] = stage[c, :, at:at + n]

    pl.semaphore_wait(barrier, len(neighbours))

    comm = Comm(g_ssem, g_rsem, sib)
    sibs = {}
    for i in (1, 2, 0, 4, 3):
        w, at, n = cols[i]
        sibs[i] = comm.send(stage.at[1 - c, :, at:at + n], sib, dst=w.at[z, y, mine])

    def own_ready(i):
        comm.wait(cols[i][0].at[z, y, other], sibs[i])

    lo, hi, full = pl.ds(0, 32), pl.ds(32, 32), pl.ds(0, 64)

    class ZthenY:
        def __init__(self, w):
            self.w = w
            self.y_sent, self.half = {}, []

        def send_z(self):
            own = self.w.at[z, y]
            self.p, self.m = comm.send(own, dzp), comm.send(own, dzm)

        def send_y(self, key):
            blk = self.w.at[(z + NZ + key) % NZ, y]
            self.y_sent[key] = (comm.send(blk, dyp), comm.send(blk, dym))

        def ring(self, d, with_y):
            w, zm, zp = self.w, (z + NZ - d) % NZ, (z + d) % NZ
            if d == 4:
                comm.wait(w.at[zp, y, lo], self.p)
                comm.wait(w.at[zp, y, hi], self.m)
                if with_y:
                    self.send_y(4)
                return
            comm.wait(w.at[zm, y], self.p)
            self.p = comm.send(w.at[zm, y, lo if d == 3 else full], dzp)
            if with_y:
                self.send_y(-d)
            comm.wait(w.at[zp, y], self.m)
            self.m = comm.send(w.at[zp, y, hi if d == 3 else full], dzm)
            if with_y:
                self.send_y(d)

        def arrive(self, *keys):
            for key in keys:
                zz = (z + NZ + key) % NZ
                i_p, i_m = self.y_sent[key]
                comm.wait(self.w.at[zz, ym], i_p)
                h_p = comm.send(self.w.at[zz, ym, lo], dyp)
                comm.wait(self.w.at[zz, yp], i_m)
                h_m = comm.send(self.w.at[zz, yp, hi], dym)
                self.half.append((zz, h_p, h_m))

        def finish(self):
            for zz, h_p, h_m in self.half:
                comm.wait(self.w.at[zz, y2, lo], h_p)
                comm.wait(self.w.at[zz, y2, hi], h_m)

    class YthenZ:
        def __init__(self, w):
            self.w = w
            self.at = {}

        def send_y(self):
            own = self.w.at[z, y]
            self.p, self.m = comm.send(own, dyp), comm.send(own, dym)

        def y_forward(self):
            w = self.w
            comm.wait(w.at[z, ym], self.p)
            self.p = comm.send(w.at[z, ym, lo], dyp)
            comm.wait(w.at[z, yp], self.m)
            self.m = comm.send(w.at[z, yp, hi], dym)

        def y_finish(self):
            comm.wait(self.w.at[z, y2, lo], self.p)
            comm.wait(self.w.at[z, y2, hi], self.m)

        def send_z(self, *ks):
            for k in ks:
                blk = self.w.at[z, (y, ym, yp, y2)[k]]
                self.at[k] = (comm.send(blk, dzp), comm.send(blk, dzm))

        def ring(self, d):
            w, zm, zp = self.w, (z + NZ - d) % NZ, (z + d) % NZ
            for k in range(4):
                yy = (y, ym, yp, y2)[k]
                p, m = self.at[k]
                if d == 4:
                    comm.wait(w.at[zp, yy, lo], p)
                    comm.wait(w.at[zp, yy, hi], m)
                    continue
                comm.wait(w.at[zm, yy], p)
                p = comm.send(w.at[zm, yy, lo if d == 3 else full], dzp)
                comm.wait(w.at[zp, yy], m)
                m = comm.send(w.at[zp, yy, hi if d == 3 else full], dzm)
                self.at[k] = (p, m)

    eye = lax.broadcasted_iota(jnp.int32, (STEP, STEP), 0) == lax.broadcasted_iota(jnp.int32, (STEP, STEP), 1)
    sign = jnp.where(lax.broadcasted_iota(jnp.int32, (1, HEAD_DIM), 1) < 64, -1.0, 1.0)

    def table(m):
        starts = jnp.broadcast_to(doc_ref[m:m + 1, :].astype(jnp.float32), (STEP, 128))
        for b in range(2):
            rows = slice(b * STEP, (b + 1) * STEP)
            at = pl.ds(pl.multiple_of(chip * ROWS + b * STEP, STEP), STEP)
            row = jnp.broadcast_to(pos_ref[m:m + 1, at].astype(jnp.float32), (STEP, STEP))
            pos = jnp.sum(jnp.where(eye, row, 0.0), axis=1, keepdims=True)
            beg = jnp.max(jnp.where(starts <= pos, starts, 0.0), axis=1, keepdims=True)
            angles = (pos - beg) * inv_ref[...]
            cos_t[m, rows, :] = jnp.cos(angles)
            sin_t[m, rows, :] = jnp.sin(angles) * sign
            qpos_t[m, rows, :] = jnp.broadcast_to(pos, (STEP, 128))
            qbeg_t[m, rows, :] = jnp.broadcast_to(beg, (STEP, 128))
        kpos_t[m] = pos_ref[m:m + 1, pl.ds(pl.multiple_of(z * 4 * ROWS, 4 * ROWS), 4 * ROWS)].astype(jnp.float32)

    def half_rows(r):
        return pl.ds(pl.multiple_of(r * STEP, STEP), STEP)

    def h_in(m, r):
        ref = hid.at[m, c, half_rows(r)]
        return rcopy(ref, ref, x_ssem.at[m, r], x_rsem.at[m, r], xprev)

    def h_fwd(m, r):
        ref = hid.at[m, c, half_rows(r)]
        return rcopy(ref, ref, d_ssem.at[m, r], d_rsem.at[m, r], sib)

    def h_fwd_in(m, r):
        ref = hid.at[m, 1 - c, half_rows(r)]
        return rcopy(ref, ref, d_ssem.at[m, r], d_rsem.at[m, r], sib)

    def kv_out(m, r, i):
        ref = kvb.at[m, y, half_rows(r)]
        return rcopy(ref, ref, k_ssem.at[m, r, i], k_rsem.at[m, r, i], (dyp, dym)[i])

    def kv_in(m, r, i):
        ref = kvb.at[m, (ym, yp)[i], half_rows(r)]
        return rcopy(ref, ref, k_ssem.at[m, r, i], k_rsem.at[m, r, i], sib)

    def quarter(r, i):
        return pl.ds(pl.multiple_of(r * STEP + i * 64, 64), 64)

    def kv_half(m, r, i):
        ref = kvb.at[m, (ym, yp)[i], quarter(r, i)]
        return rcopy(ref, ref, k_ssem.at[m, r, 2 + i], k_rsem.at[m, r, 2 + i], (dyp, dym)[i])

    def kv_half_in(m, r, i):
        ref = kvb.at[m, y2, quarter(r, i)]
        return rcopy(ref, ref, k_ssem.at[m, r, 2 + i], k_rsem.at[m, r, 2 + i], sib)

    def rope(v, cos, sin):
        return v * cos + pltpu.roll(v, 64, 1) * sin

    def hin(m, r):
        @pl.when(s > 0)
        def _():
            with jax.named_scope("hin"):
                h_in(m, r).wait_recv()
            h_fwd(m, r).start()

    def front(m, r):
        @pl.when(s > 0)
        def _():
            with jax.named_scope("hfwd"):
                h_fwd_in(m, r).wait_recv()

        with jax.named_scope("front"):
            rows = half_rows(r)
            h0 = hid[m, 0, rows]
            h1 = hid[m, 1, rows]
            f0, f1 = h0.astype(jnp.float32), h1.astype(jnp.float32)
            ms = jnp.sum(f0 * f0 + f1 * f1, axis=1, keepdims=True) * (1.0 / (2 * HALF))
            scale = lax.rsqrt(ms + EPS)
            cos = cos_t[m, rows]
            sin = sin_t[m, rows]
            kv = jnp.dot(h0, wkv[0:4].reshape(HALF, KVC), preferred_element_type=jnp.float32)
            kv += jnp.dot(h1, wkv[4:8].reshape(HALF, KVC), preferred_element_type=jnp.float32)
            kv = kv * scale
            for j in range(2):
                kvb[m, y, rows, j * 128:(j + 1) * 128] = rope(kv[:, j * 128:(j + 1) * 128], cos, sin).astype(jnp.bfloat16)
            kvb[m, y, rows, 256:512] = kv[:, 256:512].astype(jnp.bfloat16)
            kv_out(m, r, 0).start()
            kv_out(m, r, 1).start()
            scale = scale * QSCALE
            for n, w in enumerate((wq0, wq1)):
                q = jnp.dot(h0, w[0:4].reshape(HALF, 512), preferred_element_type=jnp.float32)
                q += jnp.dot(h1, w[4:8].reshape(HALF, 512), preferred_element_type=jnp.float32)
                q = q * scale
                for j in range(4):
                    h = n * 4 + j
                    qb[m, rows, h * 128:(h + 1) * 128] = rope(q[:, j * 128:(j + 1) * 128], cos, sin).astype(jnp.bfloat16)

    def kv_forward(m, r):
        with jax.named_scope("kvin"):
            for i in range(2):
                kv_in(m, r, i).wait_recv()
                kv_half(m, r, i).start()

    def a_send(m, r):
        ref = att.at[m, c, half_rows(r)]
        return rcopy(ref, ref, a_ssem.at[m, r], a_rsem.at[m, r], sib)

    def a_in(m, r):
        ref = att.at[m, 1 - c, half_rows(r)]
        return rcopy(ref, ref, a_ssem.at[m, r], a_rsem.at[m, r], sib)

    def x_send(m, r):
        return rcopy(outb.at[m, half_rows(r)], hid.at[m, c, half_rows(r)], x_ssem.at[m, r], x_rsem.at[m, r], xnext)

    out_cols = pl.ds(pl.multiple_of(c * HALF, HALF), HALF)
    out_cols_o = pl.ds(pl.multiple_of((1 - c) * HALF, HALF), HALF)

    def o_local(m):
        return pltpu.make_async_copy(outb.at[m, toks], out_ref.at[0, m, :, out_cols], l_sem.at[m])

    def o_sib(m):
        return rcopy(outb.at[m, toks_o], out_ref.at[0, m, :, out_cols], o_ssem.at[m], o_rsem.at[m], sib)

    def o_sib_in(m):
        ref = out_ref.at[0, m, :, out_cols_o]
        return rcopy(ref, ref, o_ssem.at[m], o_rsem.at[m], sib)

    def attend(m, r):
        with jax.named_scope("attn"):
            rows = half_rows(r)
            kp = kpos_t[m]
            bias = jnp.where((kp >= qbeg_t[m, rows, 0:1]) & (kp <= qpos_t[m, rows, 0:1]), 0.0, -1e30)
            ones = jnp.ones((4 * ROWS, HEAD_DIM), jnp.bfloat16)
            for h in range(8):
                j = h // 4
                k = kvb[m, :, :, j * 128:(j + 1) * 128].reshape(4 * ROWS, HEAD_DIM)
                v = kvb[m, :, :, 256 + j * 128:256 + (j + 1) * 128].reshape(4 * ROWS, HEAD_DIM)
                v = jnp.concatenate([v, ones], axis=1)
                q = qb[m, rows, h * 128:(h + 1) * 128]
                sc = lax.dot_general(q, k, (((1,), (1,)), ((), ())), preferred_element_type=jnp.float32) + bias
                mx = jnp.max(sc, axis=1, keepdims=True)
                p = jnp.exp2(sc - mx)
                o = jnp.dot(p.astype(jnp.bfloat16), v, preferred_element_type=jnp.float32)
                att[m, c, rows, h * 128:(h + 1) * 128] = (o[:, :128] / o[:, 128:]).astype(jnp.bfloat16)
            a_send(m, r).start()

    def project(m, r):
        with jax.named_scope("ain"):
            a_in(m, r).wait_recv()
        with jax.named_scope("outp"):
            rows = half_rows(r)
            for w, at, n in ((woa, 0, OAC), (wob, OAC, OBC)):
                o = jnp.dot(att[m, 0, rows], w[0:4].reshape(HALF, n), preferred_element_type=jnp.float32)
                o += jnp.dot(att[m, 1, rows], w[4:8].reshape(HALF, n), preferred_element_type=jnp.float32)
                o += hid[m, c, rows, at:at + n].astype(jnp.float32)
                outb[m, rows, at:at + n] = o.astype(jnp.bfloat16)

            @pl.when(s < SECTIONS - 1)
            def _():
                x_send(m, r).start()

            @pl.when(c != r)
            def _():
                o_sib(m).start()

            @pl.when(c == r)
            def _():
                o_local(m).start()

    first_section = s == 0
    q0_, q1_, kv_, oa_, ob_ = ZthenY(wq0), ZthenY(wq1), YthenZ(wkv), YthenZ(woa), ZthenY(wob)
    qs = (q0_, q1_)
    with jax.named_scope("flood1"):
        for i, q_ in ((1, q0_), (2, q1_)):
            own_ready(i)
            q_.send_z()
            q_.send_y(0)
        own_ready(0)
        kv_.send_y()
        own_ready(4)
        ob_.send_z()
        ob_.send_y(0)
        own_ready(3)
        oa_.send_y()
    table(0)

    @pl.when(first_section)
    def _():
        for m in range(MICRO):
            for h in range(2):
                x_local(m, h).wait()
                x_sib(m, h).start()

    def all_q(step, *args):
        for q_ in qs:
            getattr(q_, step)(*args)

    with jax.named_scope("flood2"):
        all_q("ring", 1, True)
        kv_.y_forward()
        ob_.ring(1, False)
        all_q("arrive", 0)
    with jax.named_scope("flood3"):
        all_q("ring", 2, True)
        ob_.ring(2, False)
        kv_.y_finish()
        all_q("arrive", -1, 1)
    with jax.named_scope("flood4"):
        all_q("ring", 3, True)
        kv_.send_z(0, 1, 2, 3)
        ob_.ring(3, False)
        all_q("ring", 4, True)
        ob_.ring(4, False)
        all_q("arrive", -2, 2)
        oa_.y_forward()
    table(1)
    with jax.named_scope("flood5"):
        kv_.ring(1)
        all_q("arrive", -3, 3)
    table(2)
    with jax.named_scope("flood6"):
        kv_.ring(2)
        for key in (-1, 1, -2, 2):
            ob_.send_y(key)
        all_q("arrive", 4)
        oa_.y_finish()
    table(3)
    with jax.named_scope("flood7"):
        kv_.ring(3)
        oa_.send_z(0, 1, 2, 3)
        kv_.ring(4)
        all_q("finish")

    @pl.when(first_section)
    def _():
        for m in range(MICRO):
            for h in range(2):
                x_sib_in(m, h).wait_recv()
        front(0, 0)

    with jax.named_scope("flood8"):
        for key in (-3, 3, 4):
            ob_.send_y(key)
        ob_.arrive(0, -1, 1)
        oa_.ring(1)

    @pl.when(first_section)
    def _():
        front(0, 1)

    with jax.named_scope("flood9"):
        ob_.arrive(-2, 2)
        oa_.ring(2)

    @pl.when(first_section)
    def _():
        kv_forward(0, 0)

    with jax.named_scope("flood10"):
        ob_.arrive(-3, 3, 4)
        oa_.ring(3)

    @pl.when(first_section)
    def _():
        kv_forward(0, 1)
        front(1, 0)

    with jax.named_scope("flood11"):
        oa_.ring(4)
        ob_.finish()

    @pl.when(first_section)
    def _():
        front(1, 1)
        kv_forward(1, 0)

    @pl.when(s > 0)
    def _():
        def first(r, _):
            hin(0, r)
            front(0, r)
            return 0
        lax.fori_loop(0, 2, first, 0)
        kv_forward(0, 0)

    ahead = jnp.where(first_section, 1, 0)

    def step(m, _):
        late = m + ahead
        new = late + 1

        @pl.when(late < MICRO)
        def _():
            kv_forward(late, 1)

        @pl.when(new < MICRO)
        def _():
            hin(new, 0)
            front(new, 0)
        with jax.named_scope("kvh"):
            for r in range(2):
                for i in range(2):
                    kv_half_in(m, r, i).wait_recv()
        attend(m, 0)

        @pl.when(new < MICRO)
        def _():
            hin(new, 1)
        project(m, 0)

        @pl.when(new < MICRO)
        def _():
            front(new, 1)
        attend(m, 1)

        @pl.when(new < MICRO)
        def _():
            kv_forward(new, 0)
        project(m, 1)
        return 0

    lax.fori_loop(0, MICRO, step, 0)

    with jax.named_scope("drain"):
        comm.drain()

        def settle(m, _):
            for r in range(2):
                @pl.when(s < SECTIONS - 1)
                def _():
                    x_send(m, r).wait_send()
                h_fwd(m, r).wait_send()
                for i in range(2):
                    kv_out(m, r, i).wait_send()
                    kv_half(m, r, i).wait_send()
                a_send(m, r).wait_send()
            o_local(m).wait()
            o_sib(m).wait_send()
            o_sib_in(m).wait_recv()
            return 0
        lax.fori_loop(0, MICRO, settle, 0)


def body(x_in, norm_gain, w_qkv, w_out, cycle_size, token_pos, doc_starts):
    inverse = jnp.power(jnp.float32(ROPE_BASE), -2.0 * jnp.arange(64, dtype=jnp.float32) / HEAD_DIM)
    inverse = jnp.concatenate([inverse, inverse])[None, :]
    vm = pl.BlockSpec(memory_space=pltpu.VMEM)
    anyspace = pl.BlockSpec(memory_space=pl.ANY)
    bf, f32 = jnp.bfloat16, jnp.float32
    dma = pltpu.SemaphoreType.DMA
    return pl.pallas_call(
        kernel,
        name="relay",
        out_shape=jax.ShapeDtypeStruct((1, MICRO, 128, 2 * HALF), bf),
        in_specs=[vm, vm, vm, vm, vm, vm, anyspace],
        out_specs=anyspace,
        scratch_shapes=[
            pltpu.VMEM((NZ, NY, BLK, KVC), bf), pltpu.VMEM((NZ, NY, BLK, 512), bf), pltpu.VMEM((NZ, NY, BLK, 512), bf),
            pltpu.VMEM((NZ, NY, BLK, OAC), bf), pltpu.VMEM((NZ, NY, BLK, OBC), bf),
            pltpu.VMEM((2, 32, 2560), bf),
            pltpu.VMEM((MICRO, 2, ROWS, HALF), bf),
            pltpu.VMEM((MICRO, NY, ROWS, KVC), bf),
            pltpu.VMEM((MICRO, ROWS, HALF), bf),
            pltpu.VMEM((MICRO, 2, ROWS, HALF), bf),
            pltpu.VMEM((MICRO, ROWS, HALF), bf),
            pltpu.VMEM((MICRO, ROWS, 128), f32), pltpu.VMEM((MICRO, ROWS, 128), f32),
            pltpu.VMEM((MICRO, ROWS, 128), f32), pltpu.VMEM((MICRO, ROWS, 128), f32),
            pltpu.VMEM((MICRO, 1, 4 * ROWS), f32),
            dma((N_GATHER,)), dma((N_GATHER,)),
            dma((MICRO, 2)), dma((MICRO, 2)), dma((MICRO, 2)), dma((MICRO, 2)),
            dma((MICRO, 2, 4)), dma((MICRO, 2, 4)), dma((MICRO, 2)), dma((MICRO, 2)),
            dma((MICRO,)), dma((MICRO,)), dma((MICRO,)),
        ],
        compiler_params=pltpu.CompilerParams(
            collective_id=0, has_side_effects=True, vmem_limit_bytes=60 * 1024 * 1024),
    )(w_qkv, w_out, norm_gain, token_pos, doc_starts, inverse, x_in)


def solution(mesh):
    in_specs = (P(None, "cp", None), P("pp", None), P("pp", "cp", None), P("pp", "cp", None), P(), P(), P())
    return jax.shard_map(body, mesh=mesh, in_specs=in_specs, out_specs=P("pp", None, "cp", None), check_vma=False)
```

```python
import functools
import math

import jax
import jax.numpy as jnp
from jax import lax
from jax.experimental import pallas as pl
from jax.experimental.pallas import tpu as pltpu
from jax.sharding import PartitionSpec as P

MESH = pl.DeviceIdType.MESH
HEAD_DIM = 128
MICRO = 4
SECTIONS = 4
NY = 4
NZ = 8
BLK = 64
ROWS = 256
HALF = 1024
KVC = 512
EPS = 1e-05
ROPE_BASE = 500000.0
QSCALE = HEAD_DIM ** (-0.5) * math.log2(math.e)
N_GATHER = 197
N_SEND = 40
OAC = 640
OBC = 384
STEP = 128


class Comm:
    def __init__(self, ssem, rsem, home):
        self.ssem, self.rsem, self.home = ssem, rsem, home
        self.count = 0
        self.sent = []

    def make(self, src, dst, idx, dev):
        return pltpu.make_async_remote_copy(
            src_ref=src, dst_ref=dst, send_sem=self.ssem.at[idx % N_SEND], recv_sem=self.rsem.at[idx],
            device_id=dev, device_id_type=MESH)

    def send(self, ref, dev, dst=None):
        idx = self.count
        self.count += 1
        if idx >= N_SEND:
            self.sent[idx - N_SEND].wait_send()
        copy = self.make(ref, ref if dst is None else dst, idx, dev)
        copy.start()
        self.sent.append(copy)
        return idx

    def wait(self, ref, idx):
        self.make(ref, ref, idx, self.home).wait_recv()

    def drain(self):
        for copy in self.sent[-N_SEND:]:
            copy.wait_send()
        self.sent = []


def kernel(wqkv_ref, wout_ref, gain_ref, pos_ref, doc_ref, inv_ref, x_ref, out_ref,
           wkv, wq0, wq1, woa, wob, stage, hid, kvb, qb, att, outb, cos_t, sin_t, qpos_t, qbeg_t, kpos_t,
           g_ssem, g_rsem, x_ssem, x_rsem, d_ssem, d_rsem, k_ssem, k_rsem, a_ssem, a_rsem, o_ssem, o_rsem, l_sem):
    s = lax.axis_index("pp")
    cp = lax.axis_index("cp")
    c = cp % 2
    chip = cp // 2
    y = chip % NY
    z = chip // NY
    ym, yp, y2 = (y + NY - 1) % NY, (y + 1) % NY, (y + 2) % NY

    def dev(yy, zz, cc):
        return (s, (zz * NY + yy) * 2 + cc)

    sib = dev(y, z, 1 - c)
    dyp, dym = dev(yp, z, c), dev(ym, z, c)
    dzp, dzm = dev(y, (z + 1) % NZ, c), dev(y, (z + NZ - 1) % NZ, c)
    xnext, xprev = ((s + 1) % SECTIONS, cp), ((s + SECTIONS - 1) % SECTIONS, cp)
    neighbours = (sib, dyp, dym, dzp, dzm, xnext, xprev)

    barrier = pltpu.get_barrier_semaphore()
    for d in neighbours:
        pl.semaphore_signal(barrier, inc=1, device_id=d, device_id_type=MESH)

    mine = pl.ds(pl.multiple_of(c * 32, 32), 32)
    other = pl.ds(pl.multiple_of((1 - c) * 32, 32), 32)
    toks = pl.ds(pl.multiple_of(c * STEP, STEP), STEP)
    toks_o = pl.ds(pl.multiple_of((1 - c) * STEP, STEP), STEP)

    def rcopy(src, dst, ss, rs, d):
        return pltpu.make_async_remote_copy(src_ref=src, dst_ref=dst, send_sem=ss, recv_sem=rs,
                                            device_id=d, device_id_type=MESH)

    def x_local(m, h):
        return pltpu.make_async_copy(x_ref.at[m, :, h * HALF:(h + 1) * HALF], hid.at[m, h, toks], x_rsem.at[m, h])

    def x_sib(m, h):
        return rcopy(hid.at[m, h, toks], hid.at[m, h, toks], d_ssem.at[m, h], d_rsem.at[m, h], sib)

    def x_sib_in(m, h):
        return rcopy(hid.at[m, h, toks_o], hid.at[m, h, toks_o], d_ssem.at[m, h], d_rsem.at[m, h], sib)

    @pl.when(s == 0)
    def _():
        for m in range(MICRO):
            for h in range(2):
                x_local(m, h).start()

    scope_a = jax.named_scope('stage')
    scope_a.__enter__()
    at128 = pl.ds(pl.multiple_of(cp // 4 * 128, 128), 128)
    g_row = jnp.broadcast_to(gain_ref[0:1, at128], (32, 128))
    lane = lax.broadcasted_iota(jnp.int32, (32, 128), 1)
    sub = lax.broadcasted_iota(jnp.int32, (32, 128), 0)
    g_col = jnp.sum(jnp.where(lane == sub + cp % 4 * 32, g_row, 0.0), axis=1, keepdims=True)
    for cc in range(2):
        for src_at, dst_at, n in ((2048 + 256 * cc, 0, 256), (2560 + 256 * cc, 256, 256), (HALF * cc, 512, HALF)):
            part = wqkv_ref[0, :, src_at:src_at + n].astype(jnp.float32) * g_col
            stage[cc, :, dst_at:dst_at + n] = part.astype(jnp.bfloat16)
        stage[cc, :, 1536:2560] = wout_ref[0, :, HALF * cc:HALF * (cc + 1)]
    cols = ((wkv, 0, 512), (wq0, 512, 512), (wq1, 1024, 512), (woa, 1536, OAC), (wob, 1536 + OAC, OBC))
    for w, at, n in cols:
        w[z, y, mine, :] = stage[c, :, at:at + n]

    scope_a.__exit__(None, None, None)
    with jax.named_scope('barrier'):
        pl.semaphore_wait(barrier, len(neighbours))

    comm = Comm(g_ssem, g_rsem, sib)
    sibs = {}
    for i in (1, 2, 0, 4, 3):
        w, at, n = cols[i]
        sibs[i] = comm.send(stage.at[1 - c, :, at:at + n], sib, dst=w.at[z, y, mine])

    def own_ready(i):
        comm.wait(cols[i][0].at[z, y, other], sibs[i])

    lo, hi, full = pl.ds(0, 32), pl.ds(32, 32), pl.ds(0, 64)

    class ZthenY:
        def __init__(self, w):
            self.w = w
            self.y_sent, self.half = {}, []

        def send_z(self):
            own = self.w.at[z, y]
            self.p, self.m = comm.send(own, dzp), comm.send(own, dzm)

        def send_y(self, key):
            blk = self.w.at[(z + NZ + key) % NZ, y]
            self.y_sent[key] = (comm.send(blk, dyp), comm.send(blk, dym))

        def ring(self, d, with_y):
            w, zm, zp = self.w, (z + NZ - d) % NZ, (z + d) % NZ
            if d == 4:
                comm.wait(w.at[zp, y, lo], self.p)
                comm.wait(w.at[zp, y, hi], self.m)
                if with_y:
                    self.send_y(4)
                return
            comm.wait(w.at[zm, y], self.p)
            self.p = comm.send(w.at[zm, y, lo if d == 3 else full], dzp)
            if with_y:
                self.send_y(-d)
            comm.wait(w.at[zp, y], self.m)
            self.m = comm.send(w.at[zp, y, hi if d == 3 else full], dzm)
            if with_y:
                self.send_y(d)

        def arrive(self, *keys):
            for key in keys:
                zz = (z + NZ + key) % NZ
                i_p, i_m = self.y_sent[key]
                comm.wait(self.w.at[zz, ym], i_p)
                h_p = comm.send(self.w.at[zz, ym, lo], dyp)
                comm.wait(self.w.at[zz, yp], i_m)
                h_m = comm.send(self.w.at[zz, yp, hi], dym)
                self.half.append((zz, h_p, h_m))

        def finish(self):
            for zz, h_p, h_m in self.half:
                comm.wait(self.w.at[zz, y2, lo], h_p)
                comm.wait(self.w.at[zz, y2, hi], h_m)

    class YthenZ:
        def __init__(self, w):
            self.w = w
            self.at = {}

        def send_y(self):
            own = self.w.at[z, y]
            self.p, self.m = comm.send(own, dyp), comm.send(own, dym)

        def y_forward(self):
            w = self.w
            comm.wait(w.at[z, ym], self.p)
            self.p = comm.send(w.at[z, ym, lo], dyp)
            comm.wait(w.at[z, yp], self.m)
            self.m = comm.send(w.at[z, yp, hi], dym)

        def y_finish(self):
            comm.wait(self.w.at[z, y2, lo], self.p)
            comm.wait(self.w.at[z, y2, hi], self.m)

        def send_z(self, *ks):
            for k in ks:
                blk = self.w.at[z, (y, ym, yp, y2)[k]]
                self.at[k] = (comm.send(blk, dzp), comm.send(blk, dzm))

        def ring(self, d, *ks):
            w, zm, zp = self.w, (z + NZ - d) % NZ, (z + d) % NZ
            for k in ks:
                yy = (y, ym, yp, y2)[k]
                p, m = self.at[k]
                if d == 4:
                    comm.wait(w.at[zp, yy, lo], p)
                    comm.wait(w.at[zp, yy, hi], m)
                    continue
                comm.wait(w.at[zm, yy], p)
                p = comm.send(w.at[zm, yy, lo if d == 3 else full], dzp)
                comm.wait(w.at[zp, yy], m)
                m = comm.send(w.at[zp, yy, hi if d == 3 else full], dzm)
                self.at[k] = (p, m)

    eye = lax.broadcasted_iota(jnp.int32, (STEP, STEP), 0) == lax.broadcasted_iota(jnp.int32, (STEP, STEP), 1)
    sign = jnp.where(lax.broadcasted_iota(jnp.int32, (1, HEAD_DIM), 1) < 64, -1.0, 1.0)

    def table(m):
        starts = jnp.broadcast_to(doc_ref[m:m + 1, :].astype(jnp.float32), (STEP, 128))
        for b in range(2):
            rows = slice(b * STEP, (b + 1) * STEP)
            at = pl.ds(pl.multiple_of(chip * ROWS + b * STEP, STEP), STEP)
            row = jnp.broadcast_to(pos_ref[m:m + 1, at].astype(jnp.float32), (STEP, STEP))
            pos = jnp.sum(jnp.where(eye, row, 0.0), axis=1, keepdims=True)
            beg = jnp.max(jnp.where(starts <= pos, starts, 0.0), axis=1, keepdims=True)
            angles = (pos - beg) * inv_ref[...]
            cos_t[m, rows, :] = jnp.cos(angles)
            sin_t[m, rows, :] = jnp.sin(angles) * sign
            qpos_t[m, rows, :] = jnp.broadcast_to(pos, (STEP, 128))
            qbeg_t[m, rows, :] = jnp.broadcast_to(beg, (STEP, 128))
        kpos_t[m] = pos_ref[m:m + 1, pl.ds(pl.multiple_of(z * 4 * ROWS, 4 * ROWS), 4 * ROWS)].astype(jnp.float32)

    def half_rows(r):
        return pl.ds(pl.multiple_of(r * STEP, STEP), STEP)

    def h_in(m, r):
        ref = hid.at[m, c, half_rows(r)]
        return rcopy(ref, ref, x_ssem.at[m, r], x_rsem.at[m, r], xprev)

    def h_fwd(m, r):
        ref = hid.at[m, c, half_rows(r)]
        return rcopy(ref, ref, d_ssem.at[m, r], d_rsem.at[m, r], sib)

    def h_fwd_in(m, r):
        ref = hid.at[m, 1 - c, half_rows(r)]
        return rcopy(ref, ref, d_ssem.at[m, r], d_rsem.at[m, r], sib)

    def quarter(r, i):
        return pl.ds(pl.multiple_of(r * STEP + i * 64, 64), 64)

    def kv_out(m, r, i, piece):
        ref = kvb.at[m, y, quarter(r, i if piece == 0 else 1 - i)]
        k = 2 * i + piece
        return rcopy(ref, ref, k_ssem.at[r, k], k_rsem.at[m, r, k], (dyp, dym)[i])

    def kv_in(m, r, i, piece):
        ref = kvb.at[m, (ym, yp)[i], quarter(r, i if piece == 0 else 1 - i)]
        k = 2 * i + piece
        return rcopy(ref, ref, k_ssem.at[r, k], k_rsem.at[m, r, k], sib)

    def kv_half(m, r, i):
        ref = kvb.at[m, (ym, yp)[i], quarter(r, i)]
        return rcopy(ref, ref, k_ssem.at[r, 4 + i], k_rsem.at[m, r, 4 + i], (dyp, dym)[i])

    def kv_half_in(m, r, i):
        ref = kvb.at[m, y2, quarter(r, i)]
        return rcopy(ref, ref, k_ssem.at[r, 4 + i], k_rsem.at[m, r, 4 + i], sib)

    def rope(v, cos, sin):
        return v * cos + pltpu.roll(v, 64, 1) * sin

    def hin(m, r):
        @pl.when(s > 0)
        def _():
            with jax.named_scope("hin"):
                h_in(m, r).wait_recv()
            h_fwd(m, r).start()

    def front(m, r):
        m = jnp.asarray(m, jnp.int32)
        @pl.when(s > 0)
        def _():
            with jax.named_scope("hfwd"):
                h_fwd_in(m, r).wait_recv()

        with jax.named_scope("front"):
            rows = half_rows(r)
            h0 = hid[m, 0, rows]
            h1 = hid[m, 1, rows]
            f0, f1 = h0.astype(jnp.float32), h1.astype(jnp.float32)
            ms = jnp.sum(f0 * f0 + f1 * f1, axis=1, keepdims=True) * (1.0 / (2 * HALF))
            scale = lax.rsqrt(ms + EPS)
            cos = cos_t[m, rows]
            sin = sin_t[m, rows]
            kv = jnp.dot(h0, wkv[0:4].reshape(HALF, KVC), preferred_element_type=jnp.float32)
            kv += jnp.dot(h1, wkv[4:8].reshape(HALF, KVC), preferred_element_type=jnp.float32)
            kv = kv * scale
            for j in range(2):
                kvb[m, y, rows, j * 128:(j + 1) * 128] = rope(kv[:, j * 128:(j + 1) * 128], cos, sin).astype(jnp.bfloat16)
            kvb[m, y, rows, 256:512] = kv[:, 256:512].astype(jnp.bfloat16)
            @pl.when(m > 0)
            def _():
                for i in range(2):
                    for piece in range(2):
                        kv_out(m - 1, r, i, piece).wait_send()
            for piece in range(2):
                for i in range(2):
                    kv_out(m, r, i, piece).start()
            scale = scale * QSCALE
            for n, w in enumerate((wq0, wq1)):
                q = jnp.dot(h0, w[0:4].reshape(HALF, 512), preferred_element_type=jnp.float32)
                q += jnp.dot(h1, w[4:8].reshape(HALF, 512), preferred_element_type=jnp.float32)
                q = q * scale
                for j in range(4):
                    h = n * 4 + j
                    qb[m, rows, h * 128:(h + 1) * 128] = rope(q[:, j * 128:(j + 1) * 128], cos, sin).astype(jnp.bfloat16)

    def kv_forward(m, r):
        m = jnp.asarray(m, jnp.int32)
        with jax.named_scope("kvin"):
            for i in range(2):
                kv_in(m, r, i, 0).wait_recv()

                @pl.when(m > 0)
                def _():
                    kv_half(m - 1, r, i).wait_send()
                kv_half(m, r, i).start()

    def kv_wait(m):
        for r in range(2):
            for i in range(2):
                kv_in(m, r, i, 1).wait_recv()
                kv_half_in(m, r, i).wait_recv()

    def a_send(m, r):
        ref = att.at[m, c, half_rows(r)]
        return rcopy(ref, ref, a_ssem.at[m, r], a_rsem.at[m, r], sib)

    def a_in(m, r):
        ref = att.at[m, 1 - c, half_rows(r)]
        return rcopy(ref, ref, a_ssem.at[m, r], a_rsem.at[m, r], sib)

    def x_send(m, r):
        return rcopy(outb.at[m, half_rows(r)], hid.at[m, c, half_rows(r)], x_ssem.at[m, r], x_rsem.at[m, r], xnext)

    out_cols = pl.ds(pl.multiple_of(c * HALF, HALF), HALF)
    out_cols_o = pl.ds(pl.multiple_of((1 - c) * HALF, HALF), HALF)

    def o_local(m):
        return pltpu.make_async_copy(outb.at[m, toks], out_ref.at[0, m, :, out_cols], l_sem.at[m])

    def o_sib(m):
        return rcopy(outb.at[m, toks_o], out_ref.at[0, m, :, out_cols], o_ssem.at[m], o_rsem.at[m], sib)

    def o_sib_in(m):
        ref = out_ref.at[0, m, :, out_cols_o]
        return rcopy(ref, ref, o_ssem.at[m], o_rsem.at[m], sib)

    def attend(m, r):
        with jax.named_scope("attn"):
            rows = half_rows(r)
            kp = kpos_t[m]
            bias = jnp.where((kp >= qbeg_t[m, rows, 0:1]) & (kp <= qpos_t[m, rows, 0:1]), 0.0, -1e30)
            ones = jnp.ones((4 * ROWS, HEAD_DIM), jnp.bfloat16)
            for h in range(8):
                j = h // 4
                k = kvb[m, :, :, j * 128:(j + 1) * 128].reshape(4 * ROWS, HEAD_DIM)
                v = kvb[m, :, :, 256 + j * 128:256 + (j + 1) * 128].reshape(4 * ROWS, HEAD_DIM)
                v = jnp.concatenate([v, ones], axis=1)
                q = qb[m, rows, h * 128:(h + 1) * 128]
                sc = lax.dot_general(q, k, (((1,), (1,)), ((), ())), preferred_element_type=jnp.float32) + bias
                mx = jnp.max(sc, axis=1, keepdims=True)
                p = jnp.exp2(sc - mx)
                o = jnp.dot(p.astype(jnp.bfloat16), v, preferred_element_type=jnp.float32)
                att[m, c, rows, h * 128:(h + 1) * 128] = (o[:, :128] / o[:, 128:]).astype(jnp.bfloat16)
            a_send(m, r).start()

    def project(m, r):
        with jax.named_scope("ain"):
            a_in(m, r).wait_recv()
        with jax.named_scope("outp"):
            rows = half_rows(r)
            for w, at, n in ((woa, 0, OAC), (wob, OAC, OBC)):
                o = jnp.dot(att[m, 0, rows], w[0:4].reshape(HALF, n), preferred_element_type=jnp.float32)
                o += jnp.dot(att[m, 1, rows], w[4:8].reshape(HALF, n), preferred_element_type=jnp.float32)
                o += hid[m, c, rows, at:at + n].astype(jnp.float32)
                outb[m, rows, at:at + n] = o.astype(jnp.bfloat16)

            @pl.when(s < SECTIONS - 1)
            def _():
                x_send(m, r).start()

            @pl.when(c != r)
            def _():
                o_sib(m).start()

            @pl.when(c == r)
            def _():
                o_local(m).start()

    first_section = s == 0
    q0_, q1_, kv_, oa_, ob_ = ZthenY(wq0), ZthenY(wq1), YthenZ(wkv), YthenZ(woa), ZthenY(wob)
    qs = (q0_, q1_)
    def all_q(step, *args):
        for q_ in qs:
            getattr(q_, step)(*args)

    with jax.named_scope("flood1"):
        for i, q_ in ((1, q0_), (2, q1_)):
            own_ready(i)
            q_.send_z()
            q_.send_y(0)
        own_ready(0)
        kv_.send_y()
        kv_.send_z(0)
        own_ready(4)
        ob_.send_z()
        ob_.send_y(0)
        own_ready(3)
        oa_.send_y()
    table(0)

    @pl.when(first_section)
    def _():
        for m in range(MICRO):
            for h in range(2):
                x_local(m, h).wait()
                x_sib(m, h).start()

    with jax.named_scope("flood2"):
        all_q("ring", 1, True)
        kv_.ring(1, 0)
        kv_.y_forward()
        kv_.send_z(1, 2)
        ob_.ring(1, False)
        all_q("arrive", 0)
    with jax.named_scope("flood3"):
        all_q("ring", 2, True)
        kv_.ring(2, 0)
        kv_.ring(1, 1, 2)
        ob_.ring(2, False)
        kv_.y_finish()
        kv_.send_z(3)
        all_q("arrive", -1, 1)
    with jax.named_scope("flood4"):
        all_q("ring", 3, True)
        kv_.ring(3, 0)
        kv_.ring(2, 1, 2)
        kv_.ring(1, 3)
        ob_.ring(3, False)
        all_q("arrive", -2, 2)
    table(1)
    with jax.named_scope("flood5"):
        all_q("ring", 4, True)
        kv_.ring(4, 0)
        kv_.ring(3, 1, 2)
        kv_.ring(2, 3)
        ob_.ring(4, False)
        oa_.y_forward()
        oa_.send_z(0, 1)
        all_q("arrive", -3, 3)
    table(2)
    with jax.named_scope("flood6"):
        kv_.ring(4, 1, 2)
        kv_.ring(3, 3)
        oa_.ring(1, 0, 1)
        oa_.y_finish()
        oa_.send_z(2, 3)
        all_q("arrive", 4)
        kv_.ring(4, 3)
        all_q("finish")

    def each_half(*steps):
        def both(r, _):
            for one in steps:
                one(r)
            return 0
        lax.fori_loop(0, 2, both, 0)

    @pl.when(first_section)
    def _():
        for m in range(MICRO):
            for h in range(2):
                x_sib_in(m, h).wait_recv()
        each_half(lambda r: front(0, r))

    with jax.named_scope("flood7"):
        for key in (-1, 1):
            ob_.send_y(key)
        oa_.ring(2, 0, 1)
        oa_.ring(1, 2, 3)

    @pl.when(first_section)
    def _():
        kv_forward(0, 0)

    with jax.named_scope("flood8"):
        for key in (-2, 2):
            ob_.send_y(key)
        ob_.arrive(0, -1, 1)
        oa_.ring(3, 0, 1)

    @pl.when(first_section)
    def _():
        kv_forward(0, 1)

    table(3)
    with jax.named_scope("flood9"):
        for key in (-3, 3, 4):
            ob_.send_y(key)
        oa_.ring(2, 2, 3)
        ob_.arrive(-2, 2)
        oa_.ring(4, 0, 1)

    @pl.when(first_section)
    def _():
        with jax.named_scope("kvh"):
            kv_wait(0)
        attend(0, 0)

    with jax.named_scope("flood10"):
        ob_.arrive(-3, 3, 4)
        oa_.ring(3, 2, 3)

    @pl.when(first_section)
    def _():
        attend(0, 1)
        front(1, 0)

    with jax.named_scope("flood11"):
        oa_.ring(4, 2, 3)
        ob_.finish()

    @pl.when(first_section)
    def _():
        project(0, 0)
        front(1, 1)
        project(0, 1)
        kv_forward(1, 0)
        kv_forward(1, 1)

    @pl.when(s > 0)
    def _():
        each_half(lambda r: hin(0, r), lambda r: front(0, r))
        kv_forward(0, 0)
        kv_forward(0, 1)

    def step(m, _):
        new = m + 1

        @pl.when(new < MICRO)
        def _():
            hin(new, 0)
            front(new, 0)
        with jax.named_scope("kvh"):
            kv_wait(m)
        attend(m, 0)

        @pl.when(new < MICRO)
        def _():
            hin(new, 1)
        project(m, 0)

        @pl.when(new < MICRO)
        def _():
            front(new, 1)
        attend(m, 1)

        @pl.when(new < MICRO)
        def _():
            kv_forward(new, 0)
            kv_forward(new, 1)
        project(m, 1)
        return 0

    lax.fori_loop(jnp.where(first_section, 1, 0), MICRO, step, 0)

    with jax.named_scope("drain"):
        comm.drain()

        def settle(m, _):
            for r in range(2):
                @pl.when(s < SECTIONS - 1)
                def _():
                    x_send(m, r).wait_send()
                h_fwd(m, r).wait_send()
                @pl.when(m == MICRO - 1)
                def _():
                    for i in range(2):
                        kv_out(m, r, i, 0).wait_send()
                        kv_out(m, r, i, 1).wait_send()
                        kv_half(m, r, i).wait_send()
                a_send(m, r).wait_send()
            o_local(m).wait()
            o_sib(m).wait_send()
            o_sib_in(m).wait_recv()
            return 0
        lax.fori_loop(0, MICRO, settle, 0)


def body(x_in, norm_gain, w_qkv, w_out, cycle_size, token_pos, doc_starts):
    inverse = jnp.power(jnp.float32(ROPE_BASE), -2.0 * jnp.arange(64, dtype=jnp.float32) / HEAD_DIM)
    inverse = jnp.concatenate([inverse, inverse])[None, :]
    vm = pl.BlockSpec(memory_space=pltpu.VMEM)
    anyspace = pl.BlockSpec(memory_space=pl.ANY)
    bf, f32 = jnp.bfloat16, jnp.float32
    dma = pltpu.SemaphoreType.DMA
    return pl.pallas_call(
        kernel,
        name="relay",
        out_shape=jax.ShapeDtypeStruct((1, MICRO, 128, 2 * HALF), bf),
        in_specs=[vm, vm, vm, vm, vm, vm, anyspace],
        out_specs=anyspace,
        scratch_shapes=[
            pltpu.VMEM((NZ, NY, BLK, KVC), bf), pltpu.VMEM((NZ, NY, BLK, 512), bf), pltpu.VMEM((NZ, NY, BLK, 512), bf),
            pltpu.VMEM((NZ, NY, BLK, OAC), bf), pltpu.VMEM((NZ, NY, BLK, OBC), bf),
            pltpu.VMEM((2, 32, 2560), bf),
            pltpu.VMEM((MICRO, 2, ROWS, HALF), bf),
            pltpu.VMEM((MICRO, NY, ROWS, KVC), bf),
            pltpu.VMEM((MICRO, ROWS, HALF), bf),
            pltpu.VMEM((MICRO, 2, ROWS, HALF), bf),
            pltpu.VMEM((MICRO, ROWS, HALF), bf),
            pltpu.VMEM((MICRO, ROWS, 128), f32), pltpu.VMEM((MICRO, ROWS, 128), f32),
            pltpu.VMEM((MICRO, ROWS, 128), f32), pltpu.VMEM((MICRO, ROWS, 128), f32),
            pltpu.VMEM((MICRO, 1, 4 * ROWS), f32),
            dma((N_SEND,)), dma((N_GATHER,)),
            dma((MICRO, 2)), dma((MICRO, 2)), dma((MICRO, 2)), dma((MICRO, 2)),
            dma((2, 6)), dma((MICRO, 2, 6)), dma((MICRO, 2)), dma((MICRO, 2)),
            dma((MICRO,)), dma((MICRO,)), dma((MICRO,)),
        ],
        compiler_params=pltpu.CompilerParams(
            collective_id=0, has_side_effects=True, vmem_limit_bytes=60 * 1024 * 1024),
    )(w_qkv, w_out, norm_gain, token_pos, doc_starts, inverse, x_in)


def solution(mesh):
    in_specs = (P(None, "cp", None), P("pp", None), P("pp", "cp", None), P("pp", "cp", None), P(), P(), P())
    return jax.shard_map(body, mesh=mesh, in_specs=in_specs, out_specs=P("pp", None, "cp", None), check_vma=False)
```

```python
import functools
import math

import jax
import jax.numpy as jnp
from jax import lax
from jax.experimental import pallas as pl
from jax.experimental.pallas import tpu as pltpu
from jax.sharding import PartitionSpec as P

MESH = pl.DeviceIdType.MESH
HEAD_DIM = 128
MICRO = 4
SECTIONS = 4
NY = 4
NZ = 8
BLK = 64
ROWS = 256
HALF = 1024
KVC = 512
EPS = 1e-05
ROPE_BASE = 500000.0
QSCALE = HEAD_DIM ** (-0.5) * math.log2(math.e)
N_GATHER = 197
N_SEND = 40
OAC = 640
OBC = 384
STEP = 128


class Comm:
    def __init__(self, ssem, rsem, home):
        self.ssem, self.rsem, self.home = ssem, rsem, home
        self.count = 0
        self.sent = []

    def make(self, src, dst, idx, dev):
        return pltpu.make_async_remote_copy(
            src_ref=src, dst_ref=dst, send_sem=self.ssem.at[idx % N_SEND], recv_sem=self.rsem.at[idx],
            device_id=dev, device_id_type=MESH)

    def send(self, ref, dev, dst=None):
        idx = self.count
        self.count += 1
        if idx >= N_SEND:
            self.sent[idx - N_SEND].wait_send()
        copy = self.make(ref, ref if dst is None else dst, idx, dev)
        copy.start()
        self.sent.append(copy)
        return idx

    def wait(self, ref, idx):
        self.make(ref, ref, idx, self.home).wait_recv()

    def drain(self):
        for copy in self.sent[-N_SEND:]:
            copy.wait_send()
        self.sent = []


def kernel(wqkv_ref, wout_ref, gain_ref, pos_ref, doc_ref, inv_ref, x_ref, out_ref,
           wkv, wq0, wq1, woa, wob, stage, hid, kvb, qb, att, outb, cos_t, sin_t, qpos_t, qbeg_t, kpos_t,
           g_ssem, g_rsem, x_ssem, x_rsem, d_ssem, d_rsem, k_ssem, k_rsem, a_ssem, a_rsem, o_ssem, o_rsem, l_sem):
    s = lax.axis_index("pp")
    cp = lax.axis_index("cp")
    c = cp % 2
    chip = cp // 2
    y = chip % NY
    z = chip // NY
    ym, yp, y2 = (y + NY - 1) % NY, (y + 1) % NY, (y + 2) % NY

    def dev(yy, zz, cc):
        return (s, (zz * NY + yy) * 2 + cc)

    sib = dev(y, z, 1 - c)
    dyp, dym = dev(yp, z, c), dev(ym, z, c)
    dzp, dzm = dev(y, (z + 1) % NZ, c), dev(y, (z + NZ - 1) % NZ, c)
    xnext, xprev = ((s + 1) % SECTIONS, cp), ((s + SECTIONS - 1) % SECTIONS, cp)
    neighbours = (sib, dyp, dym, dzp, dzm, xnext, xprev)

    barrier = pltpu.get_barrier_semaphore()
    for d in neighbours:
        pl.semaphore_signal(barrier, inc=1, device_id=d, device_id_type=MESH)

    mine = pl.ds(pl.multiple_of(c * 32, 32), 32)
    other = pl.ds(pl.multiple_of((1 - c) * 32, 32), 32)
    toks = pl.ds(pl.multiple_of(c * STEP, STEP), STEP)
    toks_o = pl.ds(pl.multiple_of((1 - c) * STEP, STEP), STEP)

    def rcopy(src, dst, ss, rs, d):
        return pltpu.make_async_remote_copy(src_ref=src, dst_ref=dst, send_sem=ss, recv_sem=rs,
                                            device_id=d, device_id_type=MESH)

    def x_local(m, h):
        return pltpu.make_async_copy(x_ref.at[m, :, h * HALF:(h + 1) * HALF], hid.at[m, h, toks], x_rsem.at[m, h])

    def x_sib(m, h):
        return rcopy(hid.at[m, h, toks], hid.at[m, h, toks], d_ssem.at[m, h], d_rsem.at[m, h], sib)

    def x_sib_in(m, h):
        return rcopy(hid.at[m, h, toks_o], hid.at[m, h, toks_o], d_ssem.at[m, h], d_rsem.at[m, h], sib)

    @pl.when(s == 0)
    def _():
        for m in range(MICRO):
            for h in range(2):
                x_local(m, h).start()

    scope_a = jax.named_scope('stage')
    scope_a.__enter__()
    at128 = pl.ds(pl.multiple_of(cp // 4 * 128, 128), 128)
    g_row = jnp.broadcast_to(gain_ref[0:1, at128], (32, 128))
    lane = lax.broadcasted_iota(jnp.int32, (32, 128), 1)
    sub = lax.broadcasted_iota(jnp.int32, (32, 128), 0)
    g_col = jnp.sum(jnp.where(lane == sub + cp % 4 * 32, g_row, 0.0), axis=1, keepdims=True)
    for cc in range(2):
        for src_at, dst_at, n in ((2048 + 256 * cc, 0, 256), (2560 + 256 * cc, 256, 256), (HALF * cc, 512, HALF)):
            part = wqkv_ref[0, :, src_at:src_at + n].astype(jnp.float32) * g_col
            stage[cc, :, dst_at:dst_at + n] = part.astype(jnp.bfloat16)
        stage[cc, :, 1536:2560] = wout_ref[0, :, HALF * cc:HALF * (cc + 1)]
    cols = ((wkv, 0, 512), (wq0, 512, 512), (wq1, 1024, 512), (woa, 1536, OAC), (wob, 1536 + OAC, OBC))
    for w, at, n in cols:
        w[z, y, mine, :] = stage[c, :, at:at + n]

    scope_a.__exit__(None, None, None)
    with jax.named_scope('barrier'):
        pl.semaphore_wait(barrier, len(neighbours))

    comm = Comm(g_ssem, g_rsem, sib)
    sibs = {}
    for i in (1, 2, 0, 4, 3):
        w, at, n = cols[i]
        sibs[i] = comm.send(stage.at[1 - c, :, at:at + n], sib, dst=w.at[z, y, mine])

    def own_ready(i):
        comm.wait(cols[i][0].at[z, y, other], sibs[i])

    lo, hi, full = pl.ds(0, 32), pl.ds(32, 32), pl.ds(0, 64)

    class ZthenY:
        def __init__(self, w):
            self.w = w
            self.y_sent, self.half = {}, []

        def send_z(self):
            own = self.w.at[z, y]
            self.p, self.m = comm.send(own, dzp), comm.send(own, dzm)

        def send_y(self, key):
            blk = self.w.at[(z + NZ + key) % NZ, y]
            self.y_sent[key] = (comm.send(blk, dyp), comm.send(blk, dym))

        def ring(self, d, with_y):
            w, zm, zp = self.w, (z + NZ - d) % NZ, (z + d) % NZ
            if d == 4:
                comm.wait(w.at[zp, y, lo], self.p)
                comm.wait(w.at[zp, y, hi], self.m)
                if with_y:
                    self.send_y(4)
                return
            comm.wait(w.at[zm, y], self.p)
            self.p = comm.send(w.at[zm, y, lo if d == 3 else full], dzp)
            if with_y:
                self.send_y(-d)
            comm.wait(w.at[zp, y], self.m)
            self.m = comm.send(w.at[zp, y, hi if d == 3 else full], dzm)
            if with_y:
                self.send_y(d)

        def arrive(self, *keys):
            for key in keys:
                zz = (z + NZ + key) % NZ
                i_p, i_m = self.y_sent[key]
                comm.wait(self.w.at[zz, ym], i_p)
                h_p = comm.send(self.w.at[zz, ym, lo], dyp)
                comm.wait(self.w.at[zz, yp], i_m)
                h_m = comm.send(self.w.at[zz, yp, hi], dym)
                self.half.append((zz, h_p, h_m))

        def finish(self):
            for zz, h_p, h_m in self.half:
                comm.wait(self.w.at[zz, y2, lo], h_p)
                comm.wait(self.w.at[zz, y2, hi], h_m)

    class YthenZ:
        def __init__(self, w):
            self.w = w
            self.at = {}

        def send_y(self):
            own = self.w.at[z, y]
            self.p, self.m = comm.send(own, dyp), comm.send(own, dym)

        def y_forward(self):
            w = self.w
            comm.wait(w.at[z, ym], self.p)
            self.p = comm.send(w.at[z, ym, lo], dyp)
            comm.wait(w.at[z, yp], self.m)
            self.m = comm.send(w.at[z, yp, hi], dym)

        def y_finish(self):
            comm.wait(self.w.at[z, y2, lo], self.p)
            comm.wait(self.w.at[z, y2, hi], self.m)

        def send_z(self, *ks):
            for k in ks:
                blk = self.w.at[z, (y, ym, yp, y2)[k]]
                self.at[k] = (comm.send(blk, dzp), comm.send(blk, dzm))

        def ring(self, d, *ks):
            w, zm, zp = self.w, (z + NZ - d) % NZ, (z + d) % NZ
            for k in ks:
                yy = (y, ym, yp, y2)[k]
                p, m = self.at[k]
                if d == 4:
                    comm.wait(w.at[zp, yy, lo], p)
                    comm.wait(w.at[zp, yy, hi], m)
                    continue
                comm.wait(w.at[zm, yy], p)
                p = comm.send(w.at[zm, yy, lo if d == 3 else full], dzp)
                comm.wait(w.at[zp, yy], m)
                m = comm.send(w.at[zp, yy, hi if d == 3 else full], dzm)
                self.at[k] = (p, m)

    eye = lax.broadcasted_iota(jnp.int32, (STEP, STEP), 0) == lax.broadcasted_iota(jnp.int32, (STEP, STEP), 1)
    sign = jnp.where(lax.broadcasted_iota(jnp.int32, (1, HEAD_DIM), 1) < 64, -1.0, 1.0)

    def table(m):
        starts = jnp.broadcast_to(doc_ref[m:m + 1, :].astype(jnp.float32), (STEP, 128))
        for b in range(2):
            rows = slice(b * STEP, (b + 1) * STEP)
            at = pl.ds(pl.multiple_of(chip * ROWS + b * STEP, STEP), STEP)
            row = jnp.broadcast_to(pos_ref[m:m + 1, at].astype(jnp.float32), (STEP, STEP))
            pos = jnp.sum(jnp.where(eye, row, 0.0), axis=1, keepdims=True)
            beg = jnp.max(jnp.where(starts <= pos, starts, 0.0), axis=1, keepdims=True)
            angles = (pos - beg) * inv_ref[...]
            cos_t[m, rows, :] = jnp.cos(angles)
            sin_t[m, rows, :] = jnp.sin(angles) * sign
            qpos_t[m, rows, :] = jnp.broadcast_to(pos, (STEP, 128))
            qbeg_t[m, rows, :] = jnp.broadcast_to(beg, (STEP, 128))
        kpos_t[m] = pos_ref[m:m + 1, pl.ds(pl.multiple_of(z * 4 * ROWS, 4 * ROWS), 4 * ROWS)].astype(jnp.float32)

    def half_rows(r):
        return pl.ds(pl.multiple_of(r * STEP, STEP), STEP)

    def h_in(m, r):
        ref = hid.at[m, c, half_rows(r)]
        return rcopy(ref, ref, x_ssem.at[m, r], x_rsem.at[m, r], xprev)

    def h_fwd(m, r):
        ref = hid.at[m, c, half_rows(r)]
        return rcopy(ref, ref, d_ssem.at[m, r], d_rsem.at[m, r], sib)

    def h_fwd_in(m, r):
        ref = hid.at[m, 1 - c, half_rows(r)]
        return rcopy(ref, ref, d_ssem.at[m, r], d_rsem.at[m, r], sib)

    def quarter(r, i):
        return pl.ds(pl.multiple_of(r * STEP + i * 64, 64), 64)

    def kv_out(m, r, i, piece):
        ref = kvb.at[m, y, quarter(r, i if piece == 0 else 1 - i)]
        k = 2 * i + piece
        return rcopy(ref, ref, k_ssem.at[r, k], k_rsem.at[m, r, k], (dyp, dym)[i])

    def kv_in(m, r, i, piece):
        ref = kvb.at[m, (ym, yp)[i], quarter(r, i if piece == 0 else 1 - i)]
        k = 2 * i + piece
        return rcopy(ref, ref, k_ssem.at[r, k], k_rsem.at[m, r, k], sib)

    def kv_half(m, r, i):
        ref = kvb.at[m, (ym, yp)[i], quarter(r, i)]
        return rcopy(ref, ref, k_ssem.at[r, 4 + i], k_rsem.at[m, r, 4 + i], (dyp, dym)[i])

    def kv_half_in(m, r, i):
        ref = kvb.at[m, y2, quarter(r, i)]
        return rcopy(ref, ref, k_ssem.at[r, 4 + i], k_rsem.at[m, r, 4 + i], sib)

    def rope(v, cos, sin):
        return v * cos + pltpu.roll(v, 64, 1) * sin

    def hin(m, r):
        @pl.when(s > 0)
        def _():
            with jax.named_scope("hin"):
                h_in(m, r).wait_recv()
            h_fwd(m, r).start()

    def front(m, r):
        m = jnp.asarray(m, jnp.int32)
        @pl.when(s > 0)
        def _():
            with jax.named_scope("hfwd"):
                h_fwd_in(m, r).wait_recv()

        with jax.named_scope("front"):
            rows = half_rows(r)
            h0 = hid[m, 0, rows]
            h1 = hid[m, 1, rows]
            f0, f1 = h0.astype(jnp.float32), h1.astype(jnp.float32)
            ms = jnp.sum(f0 * f0 + f1 * f1, axis=1, keepdims=True) * (1.0 / (2 * HALF))
            scale = lax.rsqrt(ms + EPS)
            cos = cos_t[m, rows]
            sin = sin_t[m, rows]
            kv = jnp.dot(h0, wkv[0:4].reshape(HALF, KVC), preferred_element_type=jnp.float32)
            kv += jnp.dot(h1, wkv[4:8].reshape(HALF, KVC), preferred_element_type=jnp.float32)
            kv = kv * scale
            for j in range(2):
                kvb[m, y, rows, j * 128:(j + 1) * 128] = rope(kv[:, j * 128:(j + 1) * 128], cos, sin).astype(jnp.bfloat16)
            kvb[m, y, rows, 256:512] = kv[:, 256:512].astype(jnp.bfloat16)
            @pl.when(m > 0)
            def _():
                for i in range(2):
                    for piece in range(2):
                        kv_out(m - 1, r, i, piece).wait_send()
            for piece in range(2):
                for i in range(2):
                    kv_out(m, r, i, piece).start()
            scale = scale * QSCALE
            for n, w in enumerate((wq0, wq1)):
                q = jnp.dot(h0, w[0:4].reshape(HALF, 512), preferred_element_type=jnp.float32)
                q += jnp.dot(h1, w[4:8].reshape(HALF, 512), preferred_element_type=jnp.float32)
                q = q * scale
                for j in range(4):
                    h = n * 4 + j
                    qb[m, rows, h * 128:(h + 1) * 128] = rope(q[:, j * 128:(j + 1) * 128], cos, sin).astype(jnp.bfloat16)

    def kv_forward(m, r):
        m = jnp.asarray(m, jnp.int32)
        with jax.named_scope("kvin"):
            for i in range(2):
                kv_in(m, r, i, 0).wait_recv()

                @pl.when(m > 0)
                def _():
                    kv_half(m - 1, r, i).wait_send()
                kv_half(m, r, i).start()

    def kv_wait(m):
        for r in range(2):
            for i in range(2):
                kv_in(m, r, i, 1).wait_recv()
                kv_half_in(m, r, i).wait_recv()

    def a_send(m, r):
        ref = att.at[m, c, half_rows(r)]
        return rcopy(ref, ref, a_ssem.at[m, r], a_rsem.at[m, r], sib)

    def a_in(m, r):
        ref = att.at[m, 1 - c, half_rows(r)]
        return rcopy(ref, ref, a_ssem.at[m, r], a_rsem.at[m, r], sib)

    def x_send(m, r):
        return rcopy(outb.at[m, half_rows(r)], hid.at[m, c, half_rows(r)], x_ssem.at[m, r], x_rsem.at[m, r], xnext)

    out_cols = pl.ds(pl.multiple_of(c * HALF, HALF), HALF)
    out_cols_o = pl.ds(pl.multiple_of((1 - c) * HALF, HALF), HALF)

    def o_local(m):
        return pltpu.make_async_copy(outb.at[m, toks], out_ref.at[0, m, :, out_cols], l_sem.at[m])

    def o_sib(m):
        return rcopy(outb.at[m, toks_o], out_ref.at[0, m, :, out_cols], o_ssem.at[m], o_rsem.at[m], sib)

    def o_sib_in(m):
        ref = out_ref.at[0, m, :, out_cols_o]
        return rcopy(ref, ref, o_ssem.at[m], o_rsem.at[m], sib)

    def attend(m, r):
        with jax.named_scope("attn"):
            rows = half_rows(r)
            kp = kpos_t[m]
            bias = jnp.where((kp >= qbeg_t[m, rows, 0:1]) & (kp <= qpos_t[m, rows, 0:1]), 0.0, -1e30)
            ones = jnp.ones((4 * ROWS, HEAD_DIM), jnp.bfloat16)
            for h in range(8):
                j = h // 4
                k = kvb[m, :, :, j * 128:(j + 1) * 128].reshape(4 * ROWS, HEAD_DIM)
                v = kvb[m, :, :, 256 + j * 128:256 + (j + 1) * 128].reshape(4 * ROWS, HEAD_DIM)
                v = jnp.concatenate([v, ones], axis=1)
                q = qb[m, rows, h * 128:(h + 1) * 128]
                sc = lax.dot_general(q, k, (((1,), (1,)), ((), ())), preferred_element_type=jnp.float32) + bias
                mx = jnp.max(sc, axis=1, keepdims=True)
                p = jnp.exp2(sc - mx)
                o = jnp.dot(p.astype(jnp.bfloat16), v, preferred_element_type=jnp.float32)
                att[m, c, rows, h * 128:(h + 1) * 128] = (o[:, :128] / o[:, 128:]).astype(jnp.bfloat16)
            a_send(m, r).start()

    def project(m, r):
        with jax.named_scope("ain"):
            a_in(m, r).wait_recv()
        with jax.named_scope("outp"):
            rows = half_rows(r)
            for w, at, n in ((woa, 0, OAC), (wob, OAC, OBC)):
                o = jnp.dot(att[m, 0, rows], w[0:4].reshape(HALF, n), preferred_element_type=jnp.float32)
                o += jnp.dot(att[m, 1, rows], w[4:8].reshape(HALF, n), preferred_element_type=jnp.float32)
                o += hid[m, c, rows, at:at + n].astype(jnp.float32)
                outb[m, rows, at:at + n] = o.astype(jnp.bfloat16)

            @pl.when(s < SECTIONS - 1)
            def _():
                x_send(m, r).start()

            @pl.when(c != r)
            def _():
                o_sib(m).start()

            @pl.when(c == r)
            def _():
                o_local(m).start()

    first_section = s == 0
    q0_, q1_, kv_, oa_, ob_ = ZthenY(wq0), ZthenY(wq1), YthenZ(wkv), YthenZ(woa), ZthenY(wob)
    qs = (q0_, q1_)
    def all_q(step, *args):
        for q_ in qs:
            getattr(q_, step)(*args)

    with jax.named_scope("flood1"):
        for i, q_ in ((1, q0_), (2, q1_)):
            own_ready(i)
            q_.send_z()
            q_.send_y(0)
        own_ready(0)
        kv_.send_y()
        kv_.send_z(0)
        own_ready(4)
        ob_.send_z()
        ob_.send_y(0)
        own_ready(3)
        oa_.send_y()
    table(0)

    @pl.when(first_section)
    def _():
        for m in range(MICRO):
            for h in range(2):
                x_local(m, h).wait()
                x_sib(m, h).start()

    with jax.named_scope("flood2"):
        all_q("ring", 1, True)
        kv_.ring(1, 0)
        kv_.y_forward()
        kv_.send_z(1, 2)
        ob_.ring(1, False)
        all_q("arrive", 0)
    with jax.named_scope("flood3"):
        all_q("ring", 2, True)
        kv_.ring(2, 0)
        kv_.ring(1, 1, 2)
        ob_.ring(2, False)
        kv_.y_finish()
        kv_.send_z(3)
        all_q("arrive", -1, 1)
    with jax.named_scope("flood4"):
        all_q("ring", 3, True)
        kv_.ring(3, 0)
        kv_.ring(2, 1, 2)
        kv_.ring(1, 3)
        ob_.ring(3, False)
        all_q("arrive", -2, 2)
    table(1)
    with jax.named_scope("flood5"):
        all_q("ring", 4, True)
        kv_.ring(4, 0)
        kv_.ring(3, 1, 2)
        kv_.ring(2, 3)
        ob_.ring(4, False)
        oa_.y_forward()
        oa_.send_z(0, 1)
        all_q("arrive", -3, 3)
    table(2)
    with jax.named_scope("flood6"):
        kv_.ring(4, 1, 2)
        kv_.ring(3, 3)
        oa_.ring(1, 0, 1)
        oa_.y_finish()
        oa_.send_z(2, 3)
        all_q("arrive", 4)
        kv_.ring(4, 3)
        all_q("finish")

    def each_half(*steps):
        def both(r, _):
            for one in steps:
                one(r)
            return 0
        lax.fori_loop(0, 2, both, 0)

    @pl.when(first_section)
    def _():
        for m in range(MICRO):
            for h in range(2):
                x_sib_in(m, h).wait_recv()
        each_half(lambda r: front(0, r))

    with jax.named_scope("flood7"):
        for key in (-1, 1):
            ob_.send_y(key)
        oa_.ring(2, 0, 1)
        oa_.ring(1, 2, 3)

    @pl.when(first_section)
    def _():
        kv_forward(0, 0)

    with jax.named_scope("flood8"):
        for key in (-2, 2):
            ob_.send_y(key)
        ob_.arrive(0, -1, 1)
        oa_.ring(3, 0, 1)

    @pl.when(first_section)
    def _():
        kv_forward(0, 1)

    table(3)
    with jax.named_scope("flood9"):
        for key in (-3, 3, 4):
            ob_.send_y(key)
        oa_.ring(2, 2, 3)
        ob_.arrive(-2, 2)
        oa_.ring(4, 0, 1)

    @pl.when(first_section)
    def _():
        with jax.named_scope("kvh"):
            kv_wait(0)
        attend(0, 0)

    with jax.named_scope("flood10"):
        ob_.arrive(-3, 3, 4)
        oa_.ring(3, 2, 3)

    @pl.when(first_section)
    def _():
        attend(0, 1)
        front(1, 0)

    with jax.named_scope("flood11"):
        oa_.ring(4, 2, 3)
        ob_.finish()

    @pl.when(first_section)
    def _():
        project(0, 0)
        front(1, 1)
        project(0, 1)
        kv_forward(1, 0)
        kv_forward(1, 1)

    @pl.when(s > 0)
    def _():
        each_half(lambda r: hin(0, r), lambda r: front(0, r))
        kv_forward(0, 0)
        kv_forward(0, 1)

    def step(m, _):
        new = m + 1

        @pl.when(new < MICRO)
        def _():
            hin(new, 0)
            front(new, 0)
        with jax.named_scope("kvh"):
            kv_wait(m)
        attend(m, 0)

        @pl.when(new < MICRO)
        def _():
            hin(new, 1)
            front(new, 1)
        project(m, 0)
        attend(m, 1)

        @pl.when(new < MICRO)
        def _():
            kv_forward(new, 0)
            kv_forward(new, 1)
        project(m, 1)
        return 0

    lax.fori_loop(jnp.where(first_section, 1, 0), MICRO, step, 0)

    with jax.named_scope("drain"):
        comm.drain()

        def settle(m, _):
            for r in range(2):
                @pl.when(s < SECTIONS - 1)
                def _():
                    x_send(m, r).wait_send()
                h_fwd(m, r).wait_send()
                @pl.when(m == MICRO - 1)
                def _():
                    for i in range(2):
                        kv_out(m, r, i, 0).wait_send()
                        kv_out(m, r, i, 1).wait_send()
                        kv_half(m, r, i).wait_send()
                a_send(m, r).wait_send()
            o_local(m).wait()
            o_sib(m).wait_send()
            o_sib_in(m).wait_recv()
            return 0
        lax.fori_loop(0, MICRO, settle, 0)


def body(x_in, norm_gain, w_qkv, w_out, cycle_size, token_pos, doc_starts):
    inverse = jnp.power(jnp.float32(ROPE_BASE), -2.0 * jnp.arange(64, dtype=jnp.float32) / HEAD_DIM)
    inverse = jnp.concatenate([inverse, inverse])[None, :]
    vm = pl.BlockSpec(memory_space=pltpu.VMEM)
    anyspace = pl.BlockSpec(memory_space=pl.ANY)
    bf, f32 = jnp.bfloat16, jnp.float32
    dma = pltpu.SemaphoreType.DMA
    return pl.pallas_call(
        kernel,
        name="relay",
        out_shape=jax.ShapeDtypeStruct((1, MICRO, 128, 2 * HALF), bf),
        in_specs=[vm, vm, vm, vm, vm, vm, anyspace],
        out_specs=anyspace,
        scratch_shapes=[
            pltpu.VMEM((NZ, NY, BLK, KVC), bf), pltpu.VMEM((NZ, NY, BLK, 512), bf), pltpu.VMEM((NZ, NY, BLK, 512), bf),
            pltpu.VMEM((NZ, NY, BLK, OAC), bf), pltpu.VMEM((NZ, NY, BLK, OBC), bf),
            pltpu.VMEM((2, 32, 2560), bf),
            pltpu.VMEM((MICRO, 2, ROWS, HALF), bf),
            pltpu.VMEM((MICRO, NY, ROWS, KVC), bf),
            pltpu.VMEM((MICRO, ROWS, HALF), bf),
            pltpu.VMEM((MICRO, 2, ROWS, HALF), bf),
            pltpu.VMEM((MICRO, ROWS, HALF), bf),
            pltpu.VMEM((MICRO, ROWS, 128), f32), pltpu.VMEM((MICRO, ROWS, 128), f32),
            pltpu.VMEM((MICRO, ROWS, 128), f32), pltpu.VMEM((MICRO, ROWS, 128), f32),
            pltpu.VMEM((MICRO, 1, 4 * ROWS), f32),
            dma((N_SEND,)), dma((N_GATHER,)),
            dma((MICRO, 2)), dma((MICRO, 2)), dma((MICRO, 2)), dma((MICRO, 2)),
            dma((2, 6)), dma((MICRO, 2, 6)), dma((MICRO, 2)), dma((MICRO, 2)),
            dma((MICRO,)), dma((MICRO,)), dma((MICRO,)),
        ],
        compiler_params=pltpu.CompilerParams(
            collective_id=0, has_side_effects=True, vmem_limit_bytes=60 * 1024 * 1024),
    )(w_qkv, w_out, norm_gain, token_pos, doc_starts, inverse, x_in)


def solution(mesh):
    in_specs = (P(None, "cp", None), P("pp", None), P("pp", "cp", None), P("pp", "cp", None), P(), P(), P())
    return jax.shard_map(body, mesh=mesh, in_specs=in_specs, out_specs=P("pp", None, "cp", None), check_vma=False)
```
